256 devices in a mesh: feat: 64 (over y, z, core), samp: 4 (over x).
Axes of the slice: x: 4, y: 4, z: 8, core: 2. Of those that a mesh axis runs over, the one named last changes fastest.
Arguments:
- design: bfloat16 [14336, 65536], P('samp', 'feat'), may hold values from -0.125 to 0.125
- targets: bfloat16 [14336, 128], P('samp'), may hold values from -26 to 26
- warm_start: float32 [65536, 128], P('feat'), may hold values from -0.6 to 0.6
- active_mask: int32 [2, 65536], P(None, 'feat'), may hold values 0 or 1
- penalty_index: int32 [1], replicated, may hold values from 0 to 7
Outputs:
- coefficients: float32 [65536, 128], P('feat')
- correlations: float32 [3, 65536], P(None, 'feat')
- relative_gaps: float32 [3], replicated
- pruned_counts: float32 [2], replicated
The draws below stay inside these ranges and needn't reach their ends.
All inputs are finite; a program needn't handle non-finite values. No bound on the sum of `active_mask` on one device may be relied on, other than what follows from the above.
Results may differ from the reference program's by a relative error of at most 0.0024.
The reference program's roundings to bfloat16 on the way count: a program that leaves them out, or rounds other values in their place, can miss the bound.
Values may be sent and summed in bfloat16 or wider, within the bound.
No kernel may reach another device: no remote copies, remote signals or barrier semaphores. Data moves between devices by JAX's collectives and lax.ppermute only.
A program may use at most 64 MiB of HBM per device.

```python
import jax
import jax.numpy as jnp
from jax import lax

K = 128
ITERS = 2
NS = 14336
P_SIZE = 65536


def draw_targets(key, part):
    phase_key = jax.random.fold_in(key, 11)
    rough_key = jax.random.fold_in(key, 12)
    noise_key = jax.random.fold_in(key, 13)
    positions = jnp.arange(NS).astype(jnp.float32) / NS
    phase = jax.random.uniform(phase_key, (), jnp.float32, 0.0, 6.2831853)
    profile = jnp.exp(1.5 * jnp.sin(6.2831853 * 3.0 * positions + phase))
    rough = jax.random.uniform(rough_key, (NS, 1), jnp.float32, 0.7, 1.4)
    noise = jnp.clip(jax.random.normal(noise_key, (NS, K), jnp.float32), -4.0, 4.0)
    return (noise * profile[:, None] * rough).astype(jnp.bfloat16)


def plant(drawn, key, smallest, top_value):
    extent = drawn.shape
    index_at = [jax.random.randint(jax.random.fold_in(key, axis), (), 0, extent[axis]) for axis in range(len(extent))]
    drawn = drawn.at[tuple(index_at)].set(smallest)
    longest = extent.index(max(extent))
    index_at[longest] = (index_at[longest] + 1) % extent[longest]
    return drawn.at[tuple(index_at)].set(top_value)


def with_spikes(values, own_key, source, target, parts, factor):
    owner, partner = [(jnp.arange(values.shape[axis_at]) // (values.shape[axis_at] // parts)).reshape([-1 if axis == axis_at else 1 for axis in range(values.ndim)]) for axis_at in (source, target)]
    chosen = jax.random.permutation(own_key, parts)[partner]
    strong = (owner == chosen) | (owner == (partner + parts // 2) % parts)
    return jnp.where(strong, factor * values, values)


def levels(rng, extent, pieces, least, high):
    loudness, own = 1.0, jax.random.fold_in(rng, 6)
    for dim, blocks in pieces:
        steps = jnp.exp(jax.random.uniform(jax.random.fold_in(own, dim), (blocks,), jnp.float32, least / len(pieces), high / len(pieces)))
        loudness = loudness * jnp.repeat(steps, extent[dim] // blocks).reshape([-1 if axis == dim else 1 for axis in range(len(extent))])
    return loudness


def scatter_about(stream_key, extent, scale, reach, cuts=(), held_as=jnp.bfloat16):
    drawn = jax.random.normal(stream_key, extent, jnp.float32) * scale
    if len(cuts) > 0:
        drawn = levels(stream_key, extent, cuts, -0.22, 0.18) * drawn
    return jnp.clip(drawn, min=-reach, max=reach).astype(held_as)


def gaussian_with(stream_key, shape, spread, bound, shards, heavy, kind=jnp.bfloat16):
    result = spread * jax.random.normal(stream_key, shape, jnp.float32)
    if shards:
        result = result * levels(stream_key, shape, shards, -0.22, 0.18)
    return jnp.clip(with_spikes(result, jax.random.fold_in(stream_key, 3), *heavy), -bound, bound).astype(kind)


def setup_inputs(seed: int = 0) -> dict:
    key_list = jax.random.split(jax.random.key(seed), 6)
    design = gaussian_with(key_list[0], (NS, P_SIZE), NS ** -0.5, 0.125, ((0, 4), (1, 64)), (1, 0, 64, 4.0))
    targets = draw_targets(jax.random.fold_in(key_list[5], 71), 0)
    warm_start = scatter_about(key_list[2], (P_SIZE, K), 0.1, 0.6, ((0, 64),), jnp.float32)
    active_mask = plant((jax.random.randint(key_list[3], (ITERS, P_SIZE), 0, 4) < 3).astype(jnp.int32), jax.random.fold_in(key_list[3], 1), 0, 1)
    penalty_index = jax.random.randint(key_list[4], (1,), 0, 8).astype(jnp.int32)
    return {"design": design, "targets": targets, "warm_start": warm_start, "active_mask": active_mask, "penalty_index": penalty_index}


def group_norms(matrix):
    return jnp.sqrt(lax.optimization_barrier(jnp.sum(matrix * matrix, axis=1)))

def transpose_product(design, right_side):
    return lax.dot_general(design, right_side, (((0,), (0,)), ((), ())), preferred_element_type=jnp.float32)

def reference(design, targets, warm_start, active_mask, penalty_index):
    corr_y = transpose_product(design, targets)
    column_squares = lax.optimization_barrier(jnp.sum(jnp.square(design.astype(jnp.float32)), axis=0))
    penalty_max = jnp.max(group_norms(corr_y))
    penalty = penalty_max / (8.0 + 4.0 * penalty_index[0].astype(jnp.float32))
    step_sizes = 0.5 / (1.0 + column_squares)
    target_float = targets.astype(jnp.float32)
    current = warm_start
    correlations = []
    relative_gaps = []
    pruned_counts = []
    for iteration in range(ITERS + 1):
        current_half = current.astype(jnp.bfloat16)
        fitted = jnp.dot(design, current_half, preferred_element_type=jnp.float32)
        residual = (target_float - fitted).astype(jnp.bfloat16)
        resid_float = residual.astype(jnp.float32)
        rr_sum = jnp.sum(resid_float * resid_float)
        ry_sum = jnp.sum(resid_float * target_float)
        bn_sum = jnp.sum(group_norms(current))
        gradient = transpose_product(design, residual)
        grad_norms = group_norms(gradient)
        scale = jnp.maximum(penalty, jnp.max(grad_norms))
        correlations.append(grad_norms / scale)
        primal = 0.5 * rr_sum + penalty * bn_sum
        ratio = penalty / scale
        dual = ratio * ry_sum - 0.5 * ratio * ratio * rr_sum
        relative_gaps.append((primal - dual) / (primal + 1.0))
        if iteration < ITERS:
            keep = active_mask[iteration].astype(jnp.float32)
            pruned_counts.append(jnp.sum(1.0 - keep))
            moved = current + step_sizes[:, None] * gradient
            moved_norms = group_norms(moved)
            cutoff = step_sizes * penalty
            factor = jnp.maximum(moved_norms - cutoff, 0.0) / jnp.maximum(moved_norms, cutoff)
            current = (keep * factor)[:, None] * moved
    return (current, jnp.stack(correlations), jnp.stack(relative_gaps), jnp.stack(pruned_counts))
```

```python
import jax
import jax.numpy as jnp
from jax import lax
from jax.experimental import pallas as pl
from jax.experimental.pallas import tpu as pltpu
from jax.sharding import Mesh
from jax.sharding import PartitionSpec as P

ITERS = 2
FEAT = ("y", "z", "core")
PLANE = ("y", "z")
ALL = ("y", "z", "core", "samp")
BF = jnp.bfloat16
F32 = jnp.float32
STEP = 448


def shifted(value, axis, by):
    n = lax.axis_size(axis)
    return lax.ppermute(value, axis, [(i, (i + by) % n) for i in range(n)])


def lane(row, index, value):
    at = lax.broadcasted_iota(jnp.int32, row.shape, 1)
    return jnp.where(at == index, value, row)


def fit_body(spec, design, c0, c1, c2, c3, out):
    total = None
    for k, block in enumerate((c0, c1, c2, c3)):
        start = pl.multiple_of(spec[1 + k] * c0.shape[1], 256)
        part = lax.dot_general(
            design[:, pl.ds(start, c0.shape[1])],
            block[...].astype(BF),
            (((1,), (1,)), ((), ())),
            preferred_element_type=F32,
        )
        total = part if total is None else total + part
    out[...] = total


def fit_rows(spec, design, blocks, rows):
    cols = design.shape[1]
    tasks, width = blocks[0].shape
    whole = pl.BlockSpec((tasks, width), lambda i, s: (0, 0))
    return pl.pallas_call(
        fit_body,
        out_shape=jax.ShapeDtypeStruct((rows, tasks), F32),
        grid_spec=pltpu.PrefetchScalarGridSpec(
            num_scalar_prefetch=1,
            grid=(rows // STEP,),
            in_specs=[pl.BlockSpec((STEP, cols), lambda i, s: (s[0] + i, 0))] + [whole] * 4,
            out_specs=pl.BlockSpec((STEP, tasks), lambda i, s: (i, 0)),
        ),
        name="fit_rows",
    )(spec, design, *blocks)


def fit_first_body(spec, design, warm, out):
    out[...] = jnp.dot(design[...], warm[...].astype(BF), preferred_element_type=F32)


def fit_first(spec, design, warm, rows):
    cols = design.shape[1]
    return pl.pallas_call(
        fit_first_body,
        out_shape=jax.ShapeDtypeStruct((rows, warm.shape[1]), F32),
        grid_spec=pltpu.PrefetchScalarGridSpec(
            num_scalar_prefetch=1,
            grid=(rows // STEP,),
            in_specs=[
                pl.BlockSpec((STEP, cols), lambda i, s: (s[0] + i, 0)),
                pl.BlockSpec(warm.shape, lambda i, s: (0, 0)),
            ],
            out_specs=pl.BlockSpec((STEP, warm.shape[1]), lambda i, s: (i, 0)),
        ),
        name="fit_first",
    )(spec, design, warm)


def grad_body(has_start, spec, right, design, *refs):
    out = refs[-1]
    width = out.shape[2]

    @pl.when(pl.program_id(0) == 0)
    def _():
        out[...] = refs[0][...] if has_start else jnp.zeros_like(out)

    turned = right[...]
    for k in range(4):
        start = pl.multiple_of(spec[1 + k] * width, 256)
        out[k] += lax.dot_general(
            turned,
            design[:, pl.ds(start, width)],
            (((0,), (0,)), ((), ())),
            preferred_element_type=F32,
        )


def grad_rows(spec, design, right, start=None):
    cols = design.shape[1]
    rows, tasks = right.shape
    shape = (4, tasks, cols // 4)
    whole = pl.BlockSpec(shape, lambda i, s: (0, 0, 0))
    extra = [] if start is None else [start]

    def body(*refs):
        grad_body(start is not None, *refs)

    return pl.pallas_call(
        body,
        out_shape=jax.ShapeDtypeStruct(shape, F32),
        grid_spec=pltpu.PrefetchScalarGridSpec(
            num_scalar_prefetch=1,
            grid=(rows // STEP,),
            in_specs=[
                pl.BlockSpec((STEP, tasks), lambda i, s: (i, 0)),
                pl.BlockSpec((STEP, cols), lambda i, s: (s[0] + i, 0)),
            ]
            + [whole] * len(extra),
            out_specs=whole,
        ),
        name="grad_rows",
    )(spec, right, design, *extra)


def corr_body(spec, right, design, out):
    width = design.shape[1] // 4
    tasks = right.shape[1]

    @pl.when(pl.program_id(0) == 0)
    def _():
        out[...] = jnp.zeros_like(out)

    turned = right[...]
    for k in range(4):
        start = pl.multiple_of(spec[1 + k] * width, 256)
        block = design[:, pl.ds(start, width)]
        out[k, :tasks] += lax.dot_general(
            turned, block, (((0,), (0,)), ((), ())), preferred_element_type=F32
        )
        wide = block.astype(F32)
        squares = (wide * wide).reshape(STEP // 8, 8, width)
        out[k, tasks:] += jnp.sum(squares, axis=0)


def corr_rows(spec, design, right):
    cols = design.shape[1]
    rows, tasks = right.shape
    shape = (4, tasks + 8, cols // 4)
    return pl.pallas_call(
        corr_body,
        out_shape=jax.ShapeDtypeStruct(shape, F32),
        grid_spec=pltpu.PrefetchScalarGridSpec(
            num_scalar_prefetch=1,
            grid=(rows // STEP,),
            in_specs=[
                pl.BlockSpec((STEP, tasks), lambda i, s: (i, 0)),
                pl.BlockSpec((STEP, cols), lambda i, s: (i, 0)),
            ],
            out_specs=pl.BlockSpec(shape, lambda i, s: (0, 0, 0)),
        ),
        name="corr_rows",
    )(spec, right, design)


def corr_end_body(own, r1, r2, r3, steps, top):
    tasks = own.shape[0] - 8
    both = own[...] + r1[...] + r2[...] + r3[...]
    column_squares = jnp.sum(both[tasks:], axis=0, keepdims=True)
    steps[...] = 0.5 / (1.0 + column_squares)
    corr = both[:tasks]
    norms = jnp.sqrt(jnp.sum(corr * corr, axis=0, keepdims=True))
    top[...] = jnp.full(top.shape, jnp.max(norms), F32)


def corr_end(parts):
    width = parts[0].shape[1]
    return pl.pallas_call(
        corr_end_body,
        out_shape=(
            jax.ShapeDtypeStruct((1, width), F32),
            jax.ShapeDtypeStruct((1, 128), F32),
        ),
        name="corr_end",
    )(*parts)


def residual_body(at, parts, own, stats, copies, stats_out):
    fitted = jnp.sum(parts[...].astype(F32), axis=0)
    target = own[...].astype(F32)
    rounded = (target - fitted).astype(BF)
    copies[...] = jnp.broadcast_to(rounded[None], copies.shape)
    wide = rounded.astype(F32)
    row = lane(stats[...], at, jnp.sum(wide * wide))
    stats_out[...] = lane(row, at + 1, jnp.sum(wide * target))


def residual_of(parts, own, stats, at):
    def body(*refs):
        residual_body(at, *refs)

    return pl.pallas_call(
        body,
        out_shape=(
            jax.ShapeDtypeStruct(parts.shape, BF),
            jax.ShapeDtypeStruct(stats.shape, F32),
        ),
        name="residual_of",
    )(parts, own, stats)


def lane_norms(value):
    return jnp.sqrt(jnp.sum(value * value, axis=0, keepdims=True))


def prox_body(at, out_dtype, own, r1, r2, r3, current, steps, mask, tops, index, stats,
              new, sent, norms_out, stats_out):
    gradient = own[...] + r1[...] + r2[...] + r3[...]
    norms = lane_norms(gradient)
    norms_out[...] = norms
    here = current[...]
    keep = mask[...].astype(F32)
    row = lane(stats[...], at + 2, jnp.sum(lane_norms(here)))
    row = lane(row, at + 3, jnp.max(norms))
    stats_out[...] = lane(row, at + 4, jnp.sum(1.0 - keep))
    penalty = jnp.max(tops[...]) / (8.0 + 4.0 * index[0].astype(F32))
    step = steps[...]
    moved = here + step * gradient
    moved_norms = lane_norms(moved)
    cutoff = step * penalty
    factor = jnp.maximum(moved_norms - cutoff, 0.0) / jnp.maximum(moved_norms, cutoff)
    value = (keep * factor) * moved
    new[...] = value
    sent[...] = value.astype(out_dtype)


VMEM = pl.BlockSpec(memory_space=pltpu.VMEM)
SMEM = pl.BlockSpec(memory_space=pltpu.SMEM)


def prox(parts, current, steps, mask, tops, index, stats, at, out_dtype):
    def body(*refs):
        prox_body(at, out_dtype, *refs)

    return pl.pallas_call(
        body,
        in_specs=[VMEM] * 8 + [SMEM] + [VMEM],
        out_shape=(
            jax.ShapeDtypeStruct(current.shape, F32),
            jax.ShapeDtypeStruct(current.shape, out_dtype),
            jax.ShapeDtypeStruct(steps.shape, F32),
            jax.ShapeDtypeStruct(stats.shape, F32),
        ),
        name="prox",
    )(*parts, current, steps, mask, tops, index, stats)


def last_body(at, own, r1, r2, r3, current, stats, n0, n1, norms_out, stats_out):
    gradient = own[...] + r1[...] + r2[...] + r3[...]
    norms = lane_norms(gradient)
    norms_out[...] = jnp.concatenate([n0[...], n1[...], norms] + [norms] * 5, axis=0)
    row = lane(stats[...], at + 2, jnp.sum(lane_norms(current[...])))
    stats_out[...] = lane(row, at + 3, jnp.max(norms))


def last_norms(parts, current, stats, n0, n1, at):
    def body(*refs):
        last_body(at, *refs)

    return pl.pallas_call(
        body,
        out_shape=(
            jax.ShapeDtypeStruct((8, n0.shape[1]), F32),
            jax.ShapeDtypeStruct(stats.shape, F32),
        ),
        name="last_norms",
    )(*parts, current, stats, n0, n1)


def finish_body(spec, everyone, tops, index, n0, n1, n2, n3, correlations, scalars):
    values = everyone[...]
    sums = jnp.sum(values, axis=0, keepdims=True)
    highs = jnp.max(values, axis=0, keepdims=True)
    at_lane = lax.broadcasted_iota(jnp.int32, sums.shape, 1)

    def total(i):
        return jnp.sum(jnp.where(at_lane == i, sums, 0.0))

    penalty = jnp.max(tops[...]) / (8.0 + 4.0 * index[0].astype(F32))
    width = n0.shape[1]
    row = jnp.zeros(sums.shape, F32)
    for t in range(ITERS + 1):
        at = 8 * t
        rr, ry, bn = total(at), total(at + 1), total(at + 2)
        top = jnp.max(jnp.where(at_lane == at + 3, highs, 0.0))
        scale = jnp.maximum(penalty, top)
        rr, ry, bn = (jnp.full(sums.shape, v, F32) for v in (rr, ry, bn))
        wide = jnp.full(sums.shape, scale, F32)
        ratio = penalty / wide
        primal = 0.5 * rr + penalty * bn
        dual = ratio * ry - 0.5 * ratio * ratio * rr
        row = jnp.where(at_lane == t, (primal - dual) / (primal + 1.0), row)
        for k, block in enumerate((n0, n1, n2, n3)):
            start = pl.multiple_of(spec[1 + k] * width, 256)
            correlations[t : t + 1, pl.ds(start, width)] = block[t : t + 1, :] / scale
        if t < ITERS:
            row = jnp.where(at_lane == ITERS + 1 + t, total(at + 4), row)
    scalars[...] = row


def finish(spec, everyone, tops, index, blocks):
    width = blocks[0].shape[1]
    return pl.pallas_call(
        finish_body,
        in_specs=[SMEM, VMEM, VMEM, SMEM] + [VMEM] * 4,
        out_shape=(
            jax.ShapeDtypeStruct((ITERS + 1, 4 * width), F32),
            jax.ShapeDtypeStruct((1, 128), F32),
        ),
        name="finish",
    )(spec, everyone, tops, index, *blocks)


def turn_body(spec, c0, c1, c2, c3, out):
    width = c0.shape[1]
    for k, block in enumerate((c0, c1, c2, c3)):
        start = pl.multiple_of(spec[1 + k] * width, 256)
        out[pl.ds(start, width), :] = block[...].T


def turned_back(spec, blocks):
    tasks, width = blocks[0].shape
    return pl.pallas_call(
        turn_body,
        in_specs=[SMEM] + [VMEM] * 4,
        out_shape=jax.ShapeDtypeStruct((4 * width, tasks), F32),
        name="turned_back",
    )(spec, *blocks)


def of_all(row):
    size = 1
    for axis in ALL:
        size *= lax.axis_size(axis)
    copies = jnp.broadcast_to(row[None], (size, *row.shape))
    got = lax.all_to_all(copies, ALL, split_axis=0, concat_axis=0, tiled=True)
    return got.reshape(size, row.shape[1])


def to_owners(blocks):
    return [blocks[0]] + [shifted(blocks[k], "samp", k) for k in (1, 3, 2)]


def from_owners(value):
    got = {k: shifted(value, "samp", -k) for k in (1, 3, 2)}
    return [value, got[1], got[2], got[3]]


def local(design, targets, warm_start, active_mask, penalty_index):
    rows, cols = design.shape
    half = rows // 2
    planes = lax.axis_size("y") * lax.axis_size("z")
    block = half // planes
    core = lax.axis_index("core")
    plane = lax.axis_index("y") * lax.axis_size("z") + lax.axis_index("z")
    x = lax.axis_index("samp")
    width = cols // 4
    steps_in_half = half // STEP
    order = [(x + k) % 4 for k in range(4)]
    own_spec = jnp.stack([core * steps_in_half] + order).astype(jnp.int32)
    other_spec = jnp.stack([(1 - core) * steps_in_half] + order).astype(jnp.int32)
    own_targets = lax.dynamic_slice_in_dim(targets, core * half + plane * block, block, 0)
    own_mask = lax.dynamic_slice_in_dim(active_mask, x * width, width, 1)
    current = lax.dynamic_slice_in_dim(warm_start, x * width, width, 0).T
    stats = jnp.zeros((1, 128), F32)

    blocks = None
    norms = []
    tops = steps = None
    coefficients = None
    for t in range(ITERS + 1):
        if t == 0:
            far = fit_first(other_spec, design, warm_start, half)
            arrived = shifted(far, "core", 1)
            near = fit_first(own_spec, design, warm_start, half)
        else:
            far = fit_rows(other_spec, design, blocks, half)
            arrived = shifted(far, "core", 1)
            near = fit_rows(own_spec, design, blocks, half)
        parts = (near + arrived).astype(BF).reshape(planes, block, -1)
        parts = lax.all_to_all(parts, PLANE, split_axis=0, concat_axis=0, tiled=True)
        if t == 0:
            corr = corr_rows(own_spec, design, targets)
            steps, top = corr_end(to_owners(corr))
            tops = of_all(top)
        copies, stats = residual_of(parts, own_targets, stats, 8 * t)
        near_rows = lax.all_to_all(copies, PLANE, split_axis=0, concat_axis=0, tiled=True)
        near_rows = near_rows.reshape(half, -1)
        far_rows = shifted(near_rows, "core", 1)
        grad = grad_rows(own_spec, design, near_rows)
        grad = grad_rows(other_spec, design, far_rows, grad)
        shares = to_owners(grad)
        if t < ITERS:
            out_dtype = BF if t + 1 < ITERS else F32
            current, sent, own_norms, stats = prox(
                shares, current, steps, own_mask[t : t + 1], tops, penalty_index, stats, 8 * t,
                out_dtype,
            )
            norms.append(own_norms)
            blocks = from_owners(sent)
            if t + 1 == ITERS:
                coefficients = turned_back(own_spec, blocks)
        else:
            packed, stats = last_norms(shares, current, stats, *norms, 8 * t)
    norm_blocks = from_owners(packed)
    everyone = of_all(stats)
    correlations, scalars = finish(own_spec, everyone, tops, penalty_index, norm_blocks)
    return (
        coefficients,
        correlations,
        scalars[0, : ITERS + 1],
        scalars[0, ITERS + 1 : 2 * ITERS + 1],
    )


def solution(mesh):
    torus = Mesh(
        mesh.devices.reshape(4, 8, 2, mesh.shape["samp"]), ("y", "z", "core", "samp")
    )
    in_specs = (P("samp", FEAT), P("samp", None), P(FEAT, None), P(None, FEAT), P())
    out_specs = (P(FEAT, None), P(None, FEAT), P(), P())
    return jax.shard_map(local, mesh=torus, in_specs=in_specs, out_specs=out_specs, check_vma=False)
```

```python
import jax
import jax.numpy as jnp
from jax import lax
from jax.experimental import pallas as pl
from jax.experimental.pallas import tpu as pltpu
from jax.sharding import Mesh
from jax.sharding import PartitionSpec as P

ITERS = 2
FEAT = ("y", "z", "core")
PLANE = ("y", "z")
ALL = ("y", "z", "core", "samp")
BF = jnp.bfloat16
F32 = jnp.float32
EXTRA = 8
VMEM = pl.BlockSpec(memory_space=pltpu.VMEM)
SMEM = pl.BlockSpec(memory_space=pltpu.SMEM)


def shape_of(dims, dtype=F32):
    return jax.ShapeDtypeStruct(tuple(dims), dtype)


def call(body, name, outs, *args, smem=(), smem_outs=(), scratch=(), mib=4):
    single = not isinstance(outs, (list, tuple))
    shapes = [outs] if single else list(outs)
    out_specs = [SMEM if k in smem_outs else VMEM for k in range(len(shapes))]
    return pl.pallas_call(
        body,
        out_shape=shapes[0] if single else tuple(shapes),
        in_specs=[SMEM if k in smem else VMEM for k in range(len(args))],
        out_specs=out_specs[0] if single else tuple(out_specs),
        scratch_shapes=list(scratch),
        compiler_params=pltpu.CompilerParams(vmem_limit_bytes=mib << 20),
        name=name,
    )(*args)


def shifted(value, axis, by):
    n = lax.axis_size(axis)
    return lax.ppermute(value, axis, [(i, (i + by) % n) for i in range(n)])


def lane(row, index, value):
    at = lax.broadcasted_iota(jnp.int32, row.shape, 1)
    return jnp.where(at == index, value, row)


def lane_norms(value):
    return jnp.sqrt(jnp.sum(value * value, axis=0, keepdims=True))


def in_hbm(value):
    return pltpu.with_memory_space_constraint(value, pltpu.HBM)


def half_start(near, half):
    core = lax.axis_index("core")
    return (core if near else 1 - core) * half


def block_at(k, width):
    return pl.multiple_of(((lax.axis_index("samp") + k) & 3) * width, width)


def fit_far(design, warm, targets, rows, step, block):
    count = design.shape[0] // step
    first = rows // step
    tasks = warm.shape[1]

    def body(design, warm, targets, out, held, own, arrived):
        begin = half_start(False, count // 2)
        plane = lax.axis_index("y") * lax.axis_size("z") + lax.axis_index("z")
        at = pl.multiple_of(half_start(True, rows) + plane * block, 8)
        mine = pltpu.make_async_copy(targets.at[pl.ds(at, block)], own, arrived.at[count])

        def piece(i):
            at = (begin + i) if i < first else (begin + i) & (count - 1)
            at = pl.multiple_of(at * step, step)
            return pltpu.make_async_copy(
                design.at[pl.ds(at, step)], held.at[pl.ds(at, step)], arrived.at[i]
            )

        for i in range(count):
            piece(i).start()
        mine.start()
        right = warm[...].astype(BF)
        for i in range(count):
            piece(i).wait()
            if i < first:
                at = pl.multiple_of((begin + i) * step, step)
                out[i * step : (i + 1) * step, :] = jnp.dot(
                    held[pl.ds(at, step), :], right, preferred_element_type=F32
                )
        mine.wait()

    return pl.pallas_call(
        body,
        out_shape=(
            shape_of((rows, tasks)),
            pltpu.VMEM(design.shape, design.dtype),
            shape_of((block, tasks), targets.dtype),
        ),
        in_specs=[
            pl.BlockSpec(memory_space=pltpu.HBM),
            VMEM,
            pl.BlockSpec(memory_space=pltpu.HBM),
        ],
        out_specs=(VMEM, VMEM, VMEM),
        scratch_shapes=[pltpu.SemaphoreType.DMA((count + 1,))],
        compiler_params=pltpu.CompilerParams(vmem_limit_bytes=16 << 20),
        name="fit_far",
    )(in_hbm(design), warm, in_hbm(targets))


def fit_near(design, warm, rows, step):
    cols, tasks = warm.shape
    width = cols // 4

    def body(design, warm, out, turned):
        right = warm[...].astype(BF)
        turned[...] = warm[pl.ds(block_at(0, width), width), :].T

        def one(i, carry):
            at = pl.multiple_of(half_start(True, rows) + i * step, step)
            out[pl.ds(pl.multiple_of(i * step, step), step), :] = jnp.dot(
                design[pl.ds(at, step), :], right, preferred_element_type=F32
            )
            return carry

        lax.fori_loop(0, rows // step, one, 0)

    return call(body, "fit_near", [shape_of((rows, tasks)), shape_of((tasks, width))], design, warm)


def fit_rows(near, design, blocks, rows, step):
    tasks, width = blocks[0].shape

    def body(design, c0, c1, c2, c3, out, whole):
        for k, block in enumerate((c0, c1, c2, c3)):
            whole[:, pl.ds(block_at(k, width), width)] = block[...].astype(BF)

        def one(i, carry):
            at = pl.multiple_of(half_start(near, rows) + i * step, step)
            out[pl.ds(pl.multiple_of(i * step, step), step), :] = lax.dot_general(
                design[pl.ds(at, step), :],
                whole[...],
                (((1,), (1,)), ((), ())),
                preferred_element_type=F32,
            )
            return carry

        lax.fori_loop(0, rows // step, one, 0)

    return call(
        body, "fit_rows", shape_of((rows, tasks)), design, *blocks,
        scratch=[pltpu.VMEM((tasks, 4 * width), BF)],
    )


def joined(near, arrived, planes, corr=None):
    rows, tasks = near.shape
    outs = [shape_of((planes, rows // planes, tasks), BF)]
    if corr:
        outs += [shape_of((1, corr[0].shape[1])), shape_of((EXTRA, tasks))]

    def body(near, arrived, *refs):
        out = refs[len(corr)] if corr else refs[0]
        total = near[...] + arrived[...]
        out[...] = total.reshape(out.shape).astype(BF)
        if corr:
            c0, c1, c2, c3, _, steps, top = refs
            both = c0[...] + c1[...] + c2[...] + c3[...]
            column_squares = jnp.sum(both[tasks:], axis=0, keepdims=True)
            steps[...] = 0.5 / (1.0 + column_squares)
            top[...] = jnp.full(top.shape, jnp.max(lane_norms(both[:tasks])), F32)

    return call(body, "joined", outs, near, arrived, *(corr or []))


def turned_dot(right, left):
    return lax.dot_general(right, left, (((0,), (0,)), ((), ())), preferred_element_type=F32)


def grad_loop(near, right, design, total, block):
    planes = right.shape[0]
    group = 8
    step = group * block

    def one(i, carry):
        rows = right[pl.ds(i * group, group)].astype(F32)[:, :block]
        rows = rows.reshape(step, right.shape[2]).astype(BF)
        at = pl.multiple_of(half_start(near, planes * block) + i * step, step)
        total[...] += turned_dot(rows, design[pl.ds(at, step), :])
        return carry

    lax.fori_loop(0, planes // group, one, 0)


def grad_near(design, right, block):
    def body(design, right, total):
        total[...] = jnp.zeros_like(total)
        grad_loop(True, right, design, total, block)

    out = shape_of((right.shape[2], design.shape[1]))
    return call(body, "grad_near", out, design, right)


def top_of(right, block):
    pieces = right[:, block:, :].astype(F32)
    return jnp.max(jnp.sum(pieces, axis=1))


def grad_far(design, right, start, block, near=None):
    tasks, cols = start.shape
    width = cols // 4
    extra = 0 if near is None else EXTRA

    def body(design, right, start, *refs):
        outs, total = refs[-5:-1], refs[-1]
        total[...] = start[...]
        grad_loop(False, right, design, total, block)
        for k, out in enumerate(outs):
            at = block_at(k, width)
            out[:tasks, :] = total[:, pl.ds(at, width)]
        if extra:
            top = jnp.maximum(top_of(right, block), top_of(refs[0], block))
            for out in outs:
                out[tasks:, :] = jnp.full((extra, width), top, F32)

    outs = [shape_of((tasks + extra, width))] * 4
    args = [design, right, start] + ([] if near is None else [near])
    return call(
        body, "grad_far", outs, *args, scratch=[pltpu.VMEM((tasks, cols), F32)]
    )


def corr_blocks(design, right, step):
    rows, cols = design.shape
    tasks = right.shape[1]
    width = cols // 4

    def body(design, right, o0, o1, o2, o3, total, squares):
        total[...] = jnp.zeros_like(total)
        squares[...] = jnp.zeros_like(squares)

        def one(i, carry):
            at = pl.multiple_of(i * step, step)
            total[...] += turned_dot(right[pl.ds(at, step), :], design[pl.ds(at, step), :])

            def part(j, carry):
                inner = pl.multiple_of(i * step + j * 64, 64)
                wide = design[pl.ds(inner, 64), :].astype(F32)
                squares[...] += jnp.sum((wide * wide).reshape(8, 8, cols), axis=0)
                return carry

            lax.fori_loop(0, step // 64, part, 0)
            return carry

        lax.fori_loop(0, rows // step, one, 0)
        for k, out in enumerate((o0, o1, o2, o3)):
            at = block_at(k, width)
            out[:tasks, :] = total[:, pl.ds(at, width)]
            out[tasks:, :] = squares[:, pl.ds(at, width)]

    return call(
        body, "corr_blocks", [shape_of((tasks + 8, width))] * 4, design, right,
        scratch=[pltpu.VMEM((tasks, cols), F32), pltpu.VMEM((8, cols), F32)],
    )


def residual_of(parts, own, at, stats=None, top=None):
    planes, block, tasks = parts.shape
    extra = 0 if top is None else EXTRA
    outs = [shape_of((planes, block + extra, tasks), BF), shape_of((1, 128))]

    def body(parts, own, given, copies, stats_out):
        fitted = jnp.sum(parts[...].astype(F32), axis=0)
        target = own[...].astype(F32)
        rounded = (target - fitted).astype(BF)
        wide = rounded.astype(F32)
        if extra:
            value = given[...]
            high = value.astype(BF).astype(F32)
            middle = (value - high).astype(BF).astype(F32)
            low = (value - high) - middle
            which = lax.broadcasted_iota(jnp.int32, value.shape, 0)
            tail = jnp.where(which == 0, high, jnp.where(which == 1, middle, low))
            tail = jnp.where(which < 3, tail, 0.0)
            rounded = jnp.concatenate([wide, tail], axis=0).astype(BF)
            row = jnp.zeros(stats_out.shape, F32)
        else:
            row = given[...]
        row = lane(row, at, jnp.sum(wide * wide))
        stats_out[...] = lane(row, at + 1, jnp.sum(wide * target))
        copies[...] = jnp.broadcast_to(rounded[None], copies.shape)

    return call(body, "residual_of", outs, parts, own, stats if top is None else top)


def penalty_of(top, index):
    return top / (8.0 + 4.0 * index[0].astype(F32))


def prox(parts, current, steps, mask, index, stats, at, out_dtype, tops=None):
    tasks, width = current.shape
    row_at = at // 8

    def body(own, r1, r2, r3, current, steps, mask, index, stats, *refs):
        new, sent, norms_out, stats_out, tops_out = refs[-5:]
        gradient = own[:tasks, :] + r1[:tasks, :] + r2[:tasks, :] + r3[:tasks, :]
        if tops is None:
            tops_out[...] = jnp.maximum(
                jnp.maximum(own[tasks:, :], r1[tasks:, :]),
                jnp.maximum(r2[tasks:, :], r3[tasks:, :]),
            )
        else:
            tops_out[...] = refs[0][...]
        norms = lane_norms(gradient)
        norms_out[...] = norms
        here = current[...]
        keep = mask[row_at : row_at + 1, pl.ds(block_at(0, width), width)].astype(F32)
        row = lane(stats[...], at + 2, jnp.sum(lane_norms(here)))
        row = lane(row, at + 3, jnp.max(norms))
        stats_out[...] = lane(row, at + 4, jnp.sum(1.0 - keep))
        penalty = penalty_of(tops_out[0:1, :], index)
        step = steps[...]
        moved = here + step * gradient
        moved_norms = lane_norms(moved)
        cutoff = step * penalty
        factor = jnp.maximum(moved_norms - cutoff, 0.0) / jnp.maximum(moved_norms, cutoff)
        value = (keep * factor) * moved
        new[...] = value
        sent[...] = value.astype(out_dtype)

    outs = [
        shape_of((tasks, width)),
        shape_of((tasks, width), out_dtype),
        shape_of((1, width)),
        shape_of(stats.shape),
        shape_of((EXTRA, width)),
    ]
    args = [*parts, current, steps, mask, index, stats] + ([] if tops is None else [tops])
    return call(body, "prox", outs, *args, smem=(7,))


def last_norms(parts, current, stats, n0, n1, at, devices):
    def body(own, r1, r2, r3, current, stats, n0, n1, norms_out, copies):
        norms = lane_norms(own[...] + r1[...] + r2[...] + r3[...])
        norms_out[...] = jnp.concatenate([n0[...], n1[...], norms] + [norms] * 5, axis=0)
        row = lane(stats[...], at + 2, jnp.sum(lane_norms(current[...])))
        row = lane(row, at + 3, jnp.max(norms))
        copies[...] = jnp.broadcast_to(row, copies.shape)

    outs = [shape_of((8, n0.shape[1])), shape_of((devices, stats.shape[1]))]
    return call(body, "last_norms", outs, *parts, current, stats, n0, n1)


def finish(everyone, tops, index, blocks):
    width = blocks[0].shape[1]

    def body(everyone, tops, index, n0, n1, n2, n3, correlations, gaps, counts):
        values = everyone[...]
        sums = jnp.sum(values, axis=0, keepdims=True)
        highs = jnp.max(values, axis=0, keepdims=True)
        at_lane = lax.broadcasted_iota(jnp.int32, sums.shape, 1)

        def total(i):
            return jnp.full(sums.shape, jnp.sum(jnp.where(at_lane == i, sums, 0.0)), F32)

        penalty = penalty_of(tops[0:1, 0:128], index)
        row = jnp.zeros(sums.shape, F32)
        for t in range(ITERS + 1):
            at = 8 * t
            rr, ry, bn = total(at), total(at + 1), total(at + 2)
            top = jnp.max(jnp.where(at_lane == at + 3, highs, 0.0))
            scale = jnp.maximum(penalty, top)
            ratio = penalty / scale
            primal = 0.5 * rr + penalty * bn
            dual = ratio * ry - 0.5 * ratio * ratio * rr
            row = jnp.where(at_lane == t, (primal - dual) / (primal + 1.0), row)
            wide = jnp.concatenate([scale] * (width // 128), axis=1)
            for k, block in enumerate((n0, n1, n2, n3)):
                start = block_at(k, width)
                correlations[t : t + 1, pl.ds(start, width)] = block[t : t + 1, :] / wide
        for t in range(ITERS + 1):
            gaps[t] = jnp.sum(jnp.where(at_lane == t, row, 0.0))
        for t in range(ITERS):
            counts[t] = jnp.sum(jnp.where(at_lane == 8 * t + 4, sums, 0.0))

    outs = [shape_of((ITERS + 1, 4 * width)), shape_of((ITERS + 1,)), shape_of((ITERS,))]
    return call(
        body, "finish", outs, everyone, tops, index, *blocks, smem=(2,), smem_outs=(1, 2)
    )


def turned_back(blocks):
    tasks, width = blocks[0].shape

    def body(c0, c1, c2, c3, out):
        for k, block in enumerate((c0, c1, c2, c3)):
            out[pl.ds(block_at(k, width), width), :] = block[...].T

    return call(body, "turned_back", shape_of((4 * width, tasks)), *blocks)


def to_owners(blocks):
    return [blocks[0]] + [shifted(blocks[k], "samp", k) for k in (1, 3, 2)]


def from_owners(value):
    got = {k: shifted(value, "samp", -k) for k in (1, 3, 2)}
    return [value, got[1], got[2], got[3]]


def plane_exchange(blocks):
    return lax.all_to_all(blocks, PLANE, split_axis=0, concat_axis=0, tiled=True)


def local(design, targets, warm_start, active_mask, penalty_index):
    rows, cols = design.shape
    half = rows // 2
    planes = lax.axis_size("y") * lax.axis_size("z")
    block = half // planes
    step = 8 * block
    devices = 1
    for axis in ALL:
        devices *= lax.axis_size(axis)

    blocks = tops = stats = None
    norms = []
    for t in range(ITERS + 1):
        if t == 0:
            far, design, own_targets = fit_far(design, warm_start, targets, half, step, block)
            arrived = shifted(far, "core", 1)
            near, current = fit_near(design, warm_start, half, step)
            corr = to_owners(corr_blocks(design, targets, step))
            sums, steps, top = joined(near, arrived, planes, corr)
            copies, stats = residual_of(plane_exchange(sums), own_targets, 0, top=top)
        else:
            far = fit_rows(False, design, blocks, half, step)
            arrived = shifted(far, "core", 1)
            near = fit_rows(True, design, blocks, half, step)
            (sums,) = joined(near, arrived, planes)
            copies, stats = residual_of(plane_exchange(sums), own_targets, 8 * t, stats)
        near_rows = plane_exchange(copies)
        far_rows = shifted(near_rows, "core", 1)
        grad = grad_near(design, near_rows, block)
        shares = to_owners(
            grad_far(design, far_rows, grad, block, near_rows if t == 0 else None)
        )
        if t < ITERS:
            current, sent, own_norms, stats, tops = prox(
                shares, current, steps, active_mask, penalty_index, stats, 8 * t,
                BF if t + 1 < ITERS else F32, tops,
            )
            norms.append(own_norms)
            blocks = from_owners(sent)
            if t + 1 == ITERS:
                coefficients = turned_back(blocks)
        else:
            packed, copies = last_norms(shares, current, stats, *norms, 8 * t, devices)
    norm_blocks = from_owners(packed)
    everyone = lax.all_to_all(copies[:, None, :], ALL, split_axis=0, concat_axis=0, tiled=True)
    correlations, gaps, counts = finish(
        everyone.reshape(copies.shape), tops, penalty_index, norm_blocks
    )
    return coefficients, correlations, gaps, counts


def solution(mesh):
    torus = Mesh(
        mesh.devices.reshape(4, 8, 2, mesh.shape["samp"]), ("y", "z", "core", "samp")
    )
    in_specs = (P("samp", FEAT), P("samp", None), P(FEAT, None), P(None, FEAT), P())
    out_specs = (P(FEAT, None), P(None, FEAT), P(), P())
    return jax.shard_map(local, mesh=torus, in_specs=in_specs, out_specs=out_specs, check_vma=False)
```

```python
import jax
import jax.numpy as jnp
from jax import lax
from jax.experimental import pallas as pl
from jax.experimental.pallas import tpu as pltpu
from jax.sharding import Mesh
from jax.sharding import PartitionSpec as P

ITERS = 2
FEAT = ("y", "z", "core")
ALL = ("y", "z", "core", "samp")
BF = jnp.bfloat16
F32 = jnp.float32
EXTRA = 8
VMEM = pl.BlockSpec(memory_space=pltpu.VMEM)
SMEM = pl.BlockSpec(memory_space=pltpu.SMEM)


def shape_of(dims, dtype=F32):
    return jax.ShapeDtypeStruct(tuple(dims), dtype)


def call(body, name, outs, *args, smem=(), smem_outs=(), scratch=(), mib=4):
    single = not isinstance(outs, (list, tuple))
    shapes = [outs] if single else list(outs)
    out_specs = [SMEM if k in smem_outs else VMEM for k in range(len(shapes))]
    return pl.pallas_call(
        body,
        out_shape=shapes[0] if single else tuple(shapes),
        in_specs=[SMEM if k in smem else VMEM for k in range(len(args))],
        out_specs=out_specs[0] if single else tuple(out_specs),
        scratch_shapes=list(scratch),
        compiler_params=pltpu.CompilerParams(vmem_limit_bytes=mib << 20),
        name=name,
    )(*args)


def shifted(value, axis, by):
    n = lax.axis_size(axis)
    return lax.ppermute(value, axis, [(i, (i + by) % n) for i in range(n)])


def lane(row, index, value):
    at = lax.broadcasted_iota(jnp.int32, row.shape, 1)
    return jnp.where(at == index, value, row)


def lane_norms(value):
    return jnp.sqrt(jnp.sum(value * value, axis=0, keepdims=True))


def in_hbm(value):
    return pltpu.with_memory_space_constraint(value, pltpu.HBM)


def half_start(near, half):
    core = lax.axis_index("core")
    return (core if near else 1 - core) * half


def block_at(k, width):
    return pl.multiple_of(((lax.axis_index("samp") + k) & 3) * width, width)


def corr_first(design, targets, step, mine):
    rows, cols = design.shape
    tasks = targets.shape[1]
    width = cols // 4
    count = rows // step

    def body(design, targets, o0, o1, o2, o3, held, own, total, squares, arrived):
        def piece(i):
            at = slice(i * step, (i + 1) * step)
            return pltpu.make_async_copy(design.at[at], held.at[at], arrived.at[i])

        for i in range(count):
            piece(i).start()
        at = pl.multiple_of(mine_start(rows // 2), 16)
        own[...] = targets[pl.ds(at, mine), :]
        total[...] = jnp.zeros_like(total)
        squares[...] = jnp.zeros_like(squares)
        def one(i, carry):
            here = pl.ds(pl.multiple_of(i * step, step), step)
            pltpu.make_async_copy(design.at[here], held.at[here], arrived.at[i]).wait()
            total[...] += turned_dot(targets[here, :], held[here, :])

            def part(j, carry):
                inner = pl.multiple_of(i * step + j * 64, 64)
                wide = held[pl.ds(inner, 64), :].astype(F32)
                squares[...] += jnp.sum((wide * wide).reshape(8, 8, cols), axis=0)
                return carry

            lax.fori_loop(0, step // 64, part, 0)
            return carry

        lax.fori_loop(0, count, one, 0)
        for k, out in enumerate((o0, o1, o2, o3)):
            at = block_at(k, width)
            out[:tasks, :] = total[:, pl.ds(at, width)]
            out[tasks:, :] = squares[:, pl.ds(at, width)]

    return pl.pallas_call(
        body,
        out_shape=(
            *[shape_of((tasks + 8, width))] * 4,
            pltpu.VMEM(design.shape, design.dtype),
            shape_of((mine, tasks), targets.dtype),
        ),
        in_specs=[pl.BlockSpec(memory_space=pltpu.HBM), VMEM],
        out_specs=(VMEM,) * 6,
        scratch_shapes=[
            pltpu.VMEM((tasks, cols), F32),
            pltpu.VMEM((8, cols), F32),
            pltpu.SemaphoreType.DMA((count,)),
        ],
        compiler_params=pltpu.CompilerParams(vmem_limit_bytes=16 << 20),
        name="corr_first",
    )(in_hbm(design), targets)


def mine_start(half):
    quarter = half // 4
    z_half = (lax.axis_index("z") & 1) * (quarter // 2)
    return lax.axis_index("core") * half + lax.axis_index("y") * quarter + z_half


def fit_warm(near, design, warm, rows, step):
    cols, tasks = warm.shape
    width = cols // 4

    def body(design, warm, out, *turned):
        right = warm[...].astype(BF)
        if near:
            turned[0][...] = warm[pl.ds(block_at(0, width), width), :].T

        def one(i, carry):
            at = pl.multiple_of(half_start(near, rows) + i * step, step)
            out[pl.ds(pl.multiple_of(i * step, step), step), :] = jnp.dot(
                design[pl.ds(at, step), :], right, preferred_element_type=F32
            )
            return carry

        lax.fori_loop(0, rows // step, one, 0)

    outs = [shape_of((rows, tasks))] + ([shape_of((tasks, width))] if near else [])
    return call(body, "fit_warm", outs, design, warm)


def fit_rows(near, design, blocks, rows, step):
    tasks, width = blocks[0].shape

    def body(design, c0, c1, c2, c3, out, whole):
        for k, block in enumerate((c0, c1, c2, c3)):
            whole[:, pl.ds(block_at(k, width), width)] = block[...].astype(BF)

        def one(i, carry):
            at = pl.multiple_of(half_start(near, rows) + i * step, step)
            out[pl.ds(pl.multiple_of(i * step, step), step), :] = lax.dot_general(
                design[pl.ds(at, step), :],
                whole[...],
                (((1,), (1,)), ((), ())),
                preferred_element_type=F32,
            )
            return carry

        lax.fori_loop(0, rows // step, one, 0)

    return call(
        body, "fit_rows", shape_of((rows, tasks)), design, *blocks,
        scratch=[pltpu.VMEM((tasks, 4 * width), BF)],
    )


def pieces(value):
    high = value.astype(BF).astype(F32)
    middle = (value - high).astype(BF).astype(F32)
    low = (value - high) - middle
    which = lax.broadcasted_iota(jnp.int32, value.shape, 0)
    rows = jnp.where(which == 0, high, jnp.where(which == 1, middle, low))
    rows = jnp.where(which < 3, rows, 0.0)
    return jnp.concatenate([rows, jnp.zeros_like(rows)], axis=0).astype(BF)


def top_in(tail):
    whole = jnp.sum(tail.astype(F32), axis=0, keepdims=True)
    return jnp.broadcast_to(whole, (EXTRA, whole.shape[1]))


def quarter_at(k, size):
    return pl.multiple_of(((lax.axis_index("y") + k) & 3) * size, size)


def joined(near, arrived, corr=None):
    rows, tasks = near.shape
    size = rows // 4
    extra = 16 if corr else 0
    outs = [shape_of((size, tasks))] + [shape_of((size + extra, tasks), BF)] * 3
    if corr:
        outs += [shape_of((1, corr[0].shape[1])), shape_of((EXTRA, tasks))]

    def body(near, arrived, *refs):
        if corr:
            c0, c1, c2, c3, kept, *sent, steps, top = refs
            both = c0[...] + c1[...] + c2[...] + c3[...]
            column_squares = jnp.sum(both[tasks:], axis=0, keepdims=True)
            steps[...] = 0.5 / (1.0 + column_squares)
            value = jnp.full((EXTRA, tasks), jnp.max(lane_norms(both[:tasks])), F32)
            top[...] = value
        else:
            kept, *sent = refs
        at = pl.ds(quarter_at(0, size), size)
        kept[...] = near[at, :] + arrived[at, :]
        for k, out in enumerate(sent):
            at = pl.ds(quarter_at(k + 1, size), size)
            out[:size, :] = (near[at, :] + arrived[at, :]).astype(BF)
            if corr:
                out[size:, :] = pieces(value)

    return call(body, "joined", outs, near, arrived, *(corr or []))


def halves(kept, got, top=None):
    size, tasks = kept.shape
    extra = 0 if top is None else EXTRA
    outs = [shape_of((size // 2 + extra, tasks))] * 2

    def body(kept, g1, g2, g3, *refs):
        sent, keep = refs[-2:]
        odd = lax.axis_index("z") & 1
        for out, which in ((sent, 1 - odd), (keep, odd)):
            at = pl.ds(pl.multiple_of(which * (size // 2), size // 2), size // 2)
            total = kept[at, :]
            for g in (g1, g2, g3):
                total += g[at, :].astype(F32)
            out[: size // 2, :] = total
        if extra:
            high = refs[0][...]
            for g in (g1, g2, g3):
                high = jnp.maximum(high, top_in(g[size:, :]))
            sent[size // 2 :, :] = high
            keep[size // 2 :, :] = high

    return call(body, "halves", outs, kept, *got, *([] if top is None else [top]))


def pair_sum(keep, got, size):
    def body(keep, got, out):
        out[:size, :] = keep[:size, :] + got[:size, :]
        if out.shape[0] > size:
            out[size:, :] = jnp.maximum(keep[size:, :], got[size:, :])

    return call(body, "pair_sum", shape_of(keep.shape), keep, got)


def residual_of(own, got, targets, at, stats=None):
    size, tasks = targets.shape
    extra = own.shape[0] - size
    outs = [shape_of((size, tasks), BF), shape_of((1, 128))]
    if extra:
        outs.append(shape_of((extra, tasks)))

    def body(own, g2, g6, g4, targets, *refs):
        fitted = (own[:size, :] + g4[:size, :]) + (g2[:size, :] + g6[:size, :])
        target = targets[...].astype(F32)
        rounded = (target - fitted).astype(BF)
        wide = rounded.astype(F32)
        if extra:
            out, stats_out, top = refs
            pairs = jnp.maximum(own[size:, :], g4[size:, :])
            top[...] = jnp.maximum(pairs, jnp.maximum(g2[size:, :], g6[size:, :]))
            row = jnp.zeros(stats_out.shape, F32)
        else:
            given, out, stats_out = refs
            row = given[...]
        row = lane(row, at, 0.25 * jnp.sum(wide * wide))
        stats_out[...] = lane(row, at + 1, 0.25 * jnp.sum(wide * target))
        out[...] = rounded

    return call(body, "residual_of", outs, own, *got, targets, *([] if extra else [stats]))


def quarter_of(own, got):
    size, tasks = own.shape

    def body(own, got, out):
        odd = lax.axis_index("z") & 1
        out[pl.ds(pl.multiple_of(odd * size, size), size), :] = own[...]
        out[pl.ds(pl.multiple_of((1 - odd) * size, size), size), :] = got[...]

    return call(body, "quarter_of", shape_of((2 * size, tasks), BF), own, got)


def turned_dot(right, left):
    return lax.dot_general(right, left, (((0,), (0,)), ((), ())), preferred_element_type=F32)


def gathered(quarters):
    size, tasks = quarters[0].shape

    def body(*refs):
        for k, quarter in enumerate(refs[:-1]):
            refs[-1][pl.ds(quarter_at(-k, size), size), :] = quarter[...]

    return call(body, "gathered", shape_of((4 * size, tasks), BF), *quarters)


def grad_loop(near, right, design, total):
    rows = right.shape[0]
    step = rows // 4

    def one(i, carry):
        here = pl.ds(pl.multiple_of(i * step, step), step)
        there = pl.ds(pl.multiple_of(half_start(near, rows) + i * step, step), step)
        total[...] += turned_dot(right[here, :], design[there, :])
        return carry

    lax.fori_loop(0, 4, one, 0)


def grad_near(design, right):
    def body(design, right, total):
        total[...] = jnp.zeros_like(total)
        grad_loop(True, right, design, total)

    out = shape_of((right.shape[1], design.shape[1]))
    return call(body, "grad_near", out, design, right)


def grad_far(design, right, start, tops):
    tasks, cols = start.shape
    width = cols // 4
    extra = EXTRA if tops else 0

    def body(design, right, start, *refs):
        outs, total = refs[-5:-1], refs[-1]
        total[...] = start[...]
        grad_loop(False, right, design, total)
        for k, out in enumerate(outs):
            out[:tasks, :] = total[:, pl.ds(block_at(k, width), width)]
            if extra:
                row = jnp.maximum(refs[0][...], refs[1][...])
                out[tasks:, :] = jnp.concatenate([row] * (width // row.shape[1]), axis=1)

    outs = [shape_of((tasks + extra, width))] * 4
    args = [design, right, start, *tops]
    return call(body, "grad_far", outs, *args, scratch=[pltpu.VMEM((tasks, cols), F32)])


def penalty_of(top, index):
    return top / (8.0 + 4.0 * index[0].astype(F32))


def prox(parts, current, steps, mask, index, stats, at, out_dtype, tops=None):
    tasks, width = current.shape
    row_at = at // 8

    def body(own, r1, r2, r3, current, steps, mask, index, stats, *refs):
        new, sent, norms_out, stats_out, tops_out = refs[-5:]
        gradient = own[:tasks, :] + r1[:tasks, :] + r2[:tasks, :] + r3[:tasks, :]
        if tops is None:
            tops_out[...] = jnp.maximum(
                jnp.maximum(own[tasks:, :], r1[tasks:, :]),
                jnp.maximum(r2[tasks:, :], r3[tasks:, :]),
            )
        else:
            tops_out[...] = refs[0][...]
        norms = lane_norms(gradient)
        norms_out[...] = norms
        here = current[...]
        keep = mask[row_at : row_at + 1, pl.ds(block_at(0, width), width)].astype(F32)
        row = lane(stats[...], at + 2, jnp.sum(lane_norms(here)))
        row = lane(row, at + 3, jnp.max(norms))
        stats_out[...] = lane(row, at + 4, jnp.sum(1.0 - keep))
        penalty = penalty_of(tops_out[0:1, :], index)
        step = steps[...]
        moved = here + step * gradient
        moved_norms = lane_norms(moved)
        cutoff = step * penalty
        factor = jnp.maximum(moved_norms - cutoff, 0.0) / jnp.maximum(moved_norms, cutoff)
        value = (keep * factor) * moved
        new[...] = value
        sent[...] = value.astype(out_dtype)

    outs = [
        shape_of((tasks, width)),
        shape_of((tasks, width), out_dtype),
        shape_of((1, width)),
        shape_of(stats.shape),
        shape_of((EXTRA, width)),
    ]
    args = [*parts, current, steps, mask, index, stats] + ([] if tops is None else [tops])
    return call(body, "prox", outs, *args, smem=(7,))


def last_norms(parts, current, stats, n0, n1, at, devices):
    def body(own, r1, r2, r3, current, stats, n0, n1, norms_out, copies):
        norms = lane_norms(own[...] + r1[...] + r2[...] + r3[...])
        norms_out[...] = jnp.concatenate([n0[...], n1[...], norms] + [norms] * 5, axis=0)
        row = lane(stats[...], at + 2, jnp.sum(lane_norms(current[...])))
        row = lane(row, at + 3, jnp.max(norms))
        copies[...] = jnp.broadcast_to(row, copies.shape)

    outs = [shape_of((8, n0.shape[1])), shape_of((devices, stats.shape[1]))]
    return call(body, "last_norms", outs, *parts, current, stats, n0, n1)


def finish(everyone, tops, index, blocks):
    width = blocks[0].shape[1]

    def body(everyone, tops, index, n0, n1, n2, n3, correlations, gaps, counts):
        values = everyone[...]
        sums = jnp.sum(values, axis=0, keepdims=True)
        highs = jnp.max(values, axis=0, keepdims=True)
        at_lane = lax.broadcasted_iota(jnp.int32, sums.shape, 1)

        def total(i):
            return jnp.full(sums.shape, jnp.sum(jnp.where(at_lane == i, sums, 0.0)), F32)

        penalty = penalty_of(tops[0:1, 0:128], index)
        row = jnp.zeros(sums.shape, F32)
        for t in range(ITERS + 1):
            at = 8 * t
            rr, ry, bn = total(at), total(at + 1), total(at + 2)
            top = jnp.max(jnp.where(at_lane == at + 3, highs, 0.0))
            scale = jnp.maximum(penalty, top)
            ratio = penalty / scale
            primal = 0.5 * rr + penalty * bn
            dual = ratio * ry - 0.5 * ratio * ratio * rr
            row = jnp.where(at_lane == t, (primal - dual) / (primal + 1.0), row)
            wide = jnp.concatenate([scale] * (width // 128), axis=1)
            for k, block in enumerate((n0, n1, n2, n3)):
                start = block_at(k, width)
                correlations[t : t + 1, pl.ds(start, width)] = block[t : t + 1, :] / wide
        for t in range(ITERS + 1):
            gaps[t] = jnp.sum(jnp.where(at_lane == t, row, 0.0))
        for t in range(ITERS):
            counts[t] = jnp.sum(jnp.where(at_lane == 8 * t + 4, sums, 0.0))

    outs = [shape_of((ITERS + 1, 4 * width)), shape_of((ITERS + 1,)), shape_of((ITERS,))]
    return call(
        body, "finish", outs, everyone, tops, index, *blocks, smem=(2,), smem_outs=(1, 2)
    )


def turned_back(blocks):
    tasks, width = blocks[0].shape

    def body(c0, c1, c2, c3, out):
        for k, block in enumerate((c0, c1, c2, c3)):
            out[pl.ds(block_at(k, width), width), :] = block[...].T

    return call(body, "turned_back", shape_of((4 * width, tasks)), *blocks)


def to_owners(blocks):
    return [blocks[0]] + [shifted(blocks[k], "samp", k) for k in (1, 3, 2)]


def from_owners(value):
    got = {k: shifted(value, "samp", -k) for k in (1, 3, 2)}
    return [value, got[1], got[2], got[3]]


def partner(value):
    n = lax.axis_size("z")
    return lax.ppermute(value, "z", [(i, i ^ 1) for i in range(n)])


def local(design, targets, warm_start, active_mask, penalty_index):
    rows, cols = design.shape
    half = rows // 2
    step = half // 4
    mine = step // 2
    devices = 1
    for axis in ALL:
        devices *= lax.axis_size(axis)

    blocks = stats = top = tops = None
    norms = []
    for t in range(ITERS + 1):
        first = t == 0
        if first:
            *corr, design, own_targets = corr_first(design, targets, step, mine)
            corr = to_owners(corr)
            (far,) = fit_warm(False, design, warm_start, half, step)
            arrived = shifted(far, "core", 1)
            near, current = fit_warm(True, design, warm_start, half, step)
            kept, *sent, steps, top = joined(near, arrived, corr)
        else:
            far = fit_rows(False, design, blocks, half, step)
            arrived = shifted(far, "core", 1)
            near = fit_rows(True, design, blocks, half, step)
            kept, *sent = joined(near, arrived)
            top = None
        got = [shifted(sent[k - 1], "y", k) for k in (1, 3, 2)]
        away, keep = halves(kept, got, top)
        summed = pair_sum(keep, partner(away), mine)
        got = [shifted(summed, "z", k) for k in (2, 6, 4)]
        rounded, stats, *tail = residual_of(summed, got, own_targets, 8 * t, stats)
        if first:
            tail.append(shifted(tail[0], "core", 1))
        quarter = quarter_of(rounded, partner(rounded))
        near_rows = gathered([quarter] + [shifted(quarter, "y", k) for k in (1, 2, 3)])
        far_rows = shifted(near_rows, "core", 1)
        grad = grad_near(design, near_rows)
        shares = to_owners(grad_far(design, far_rows, grad, tail))
        if t < ITERS:
            current, moved, own_norms, stats, tops = prox(
                shares, current, steps, active_mask, penalty_index, stats, 8 * t,
                BF if t + 1 < ITERS else F32, tops,
            )
            norms.append(own_norms)
            blocks = from_owners(moved)
            if t + 1 == ITERS:
                coefficients = turned_back(blocks)
        else:
            packed, copies = last_norms(shares, current, stats, *norms, 8 * t, devices)
    norm_blocks = from_owners(packed)
    everyone = lax.all_to_all(copies[:, None, :], ALL, split_axis=0, concat_axis=0, tiled=True)
    correlations, gaps, counts = finish(
        everyone.reshape(copies.shape), tops, penalty_index, norm_blocks
    )
    return coefficients, correlations, gaps, counts


def solution(mesh):
    torus = Mesh(
        mesh.devices.reshape(4, 8, 2, mesh.shape["samp"]), ("y", "z", "core", "samp")
    )
    in_specs = (P("samp", FEAT), P("samp", None), P(FEAT, None), P(None, FEAT), P())
    out_specs = (P(FEAT, None), P(None, FEAT), P(), P())
    return jax.shard_map(local, mesh=torus, in_specs=in_specs, out_specs=out_specs, check_vma=False)
```

```python
import jax
import jax.numpy as jnp
from jax import lax
from jax.experimental import pallas as pl
from jax.experimental.pallas import tpu as pltpu
from jax.sharding import Mesh
from jax.sharding import PartitionSpec as P


ITERS = 2
FEAT = ("y", "z", "core")
PLANE = ("y", "z")
BF = jnp.bfloat16
F32 = jnp.float32
EXTRA = 8
VMEM = pl.BlockSpec(memory_space=pltpu.VMEM)
SMEM = pl.BlockSpec(memory_space=pltpu.SMEM)


def shape_of(dims, dtype=F32):
    return jax.ShapeDtypeStruct(tuple(dims), dtype)


def call(body, outs, *args, smem=(), smem_outs=(), scratch=(), mib=4):
    single = not isinstance(outs, (list, tuple))
    shapes = [outs] if single else list(outs)
    out_specs = [SMEM if k in smem_outs else VMEM for k in range(len(shapes))]
    return pl.pallas_call(
        body,
        out_shape=shapes[0] if single else tuple(shapes),
        in_specs=[SMEM if k in smem else VMEM for k in range(len(args))],
        out_specs=out_specs[0] if single else tuple(out_specs),
        scratch_shapes=list(scratch),
        compiler_params=pltpu.CompilerParams(vmem_limit_bytes=mib << 20),
    )(*args)


def shifted(value, axis, by):
    n = lax.axis_size(axis)
    return lax.ppermute(value, axis, [(i, (i + by) % n) for i in range(n)])


def lane(row, index, value):
    at = lax.broadcasted_iota(jnp.int32, row.shape, 1)
    return jnp.where(at == index, value, row)


def lane_norms(value):
    return jnp.sqrt(jnp.sum(value * value, axis=0, keepdims=True))


def in_hbm(value):
    return pltpu.with_memory_space_constraint(value, pltpu.HBM)


def half_start(near, half):
    core = lax.axis_index("core")
    return (core if near else 1 - core) * half


def block_at(k, width):
    return pl.multiple_of(((lax.axis_index("samp") + k) & 3) * width, width)


def corr_first(design, targets, step, block):
    rows, cols = design.shape
    tasks = targets.shape[1]
    width = cols // 4
    count = rows // step

    def body(design, targets, o0, o1, o2, o3, held, own, right, total, squares, arrived):
        plane = lax.axis_index("y") * lax.axis_size("z") + lax.axis_index("z")
        at = pl.multiple_of(half_start(True, rows // 2) + plane * block, 8)
        mine = pltpu.make_async_copy(targets.at[pl.ds(at, block)], own, arrived.at[2 * count])

        def pieces(i):
            here = pl.ds(pl.multiple_of(i * step, step), step)
            return (
                pltpu.make_async_copy(targets.at[here], right.at[here], arrived.at[2 * i]),
                pltpu.make_async_copy(design.at[here], held.at[here], arrived.at[2 * i + 1]),
            )

        for i in range(count):
            for piece in pieces(i):
                piece.start()
        mine.start()
        total[...] = jnp.zeros_like(total)
        squares[...] = jnp.zeros_like(squares)

        def one(i, carry):
            for piece in pieces(i):
                piece.wait()
            here = pl.ds(pl.multiple_of(i * step, step), step)
            total[...] += turned_dot(right[here, :], held[here, :])

            def part(j, carry):
                inner = pl.multiple_of(i * step + j * 64, 64)
                wide = held[pl.ds(inner, 64), :].astype(F32)
                squares[...] += jnp.sum((wide * wide).reshape(8, 8, cols), axis=0)
                return carry

            lax.fori_loop(0, step // 64, part, 0)
            return carry

        lax.fori_loop(0, count, one, 0)
        mine.wait()
        for k, out in enumerate((o0, o1, o2, o3)):
            at = block_at(k, width)
            out[:tasks, :] = total[:, pl.ds(at, width)]
            out[tasks:, :] = squares[:, pl.ds(at, width)]

    hbm = pl.BlockSpec(memory_space=pltpu.HBM)
    return pl.pallas_call(
        body,
        out_shape=(
            *[shape_of((tasks + 8, width))] * 4,
            pltpu.VMEM(design.shape, design.dtype),
            shape_of((block, tasks), targets.dtype),
        ),
        in_specs=[hbm, hbm],
        out_specs=(VMEM,) * 6,
        scratch_shapes=[
            pltpu.VMEM((rows, tasks), targets.dtype),
            pltpu.VMEM((tasks, cols), F32),
            pltpu.VMEM((8, cols), F32),
            pltpu.SemaphoreType.DMA((2 * count + 1,)),
        ],
        compiler_params=pltpu.CompilerParams(vmem_limit_bytes=16 << 20),
        name="corr_first",
    )(in_hbm(design), in_hbm(targets))


def fit_warm(near, design, warm, rows, step):
    cols, tasks = warm.shape
    width = cols // 4

    def body(design, warm, out, *turned):
        right = warm[...].astype(BF)
        if near:
            turned[0][...] = warm[pl.ds(block_at(0, width), width), :].T

        def one(i, carry):
            at = pl.multiple_of(half_start(near, rows) + i * step, step)
            out[pl.ds(pl.multiple_of(i * step, step), step), :] = jnp.dot(
                design[pl.ds(at, step), :], right, preferred_element_type=F32
            )
            return carry

        lax.fori_loop(0, rows // step, one, 0)

    outs = [shape_of((rows, tasks))] + ([shape_of((tasks, width))] if near else [])
    return call(body, outs, design, warm)


def fit_rows(near, design, blocks, rows, step):
    tasks, width = blocks[0].shape

    def body(design, c0, c1, c2, c3, out, whole):
        for k, block in enumerate((c0, c1, c2, c3)):
            whole[:, pl.ds(block_at(k, width), width)] = block[...].astype(BF)

        def one(i, carry):
            at = pl.multiple_of(half_start(near, rows) + i * step, step)
            out[pl.ds(pl.multiple_of(i * step, step), step), :] = lax.dot_general(
                design[pl.ds(at, step), :],
                whole[...],
                (((1,), (1,)), ((), ())),
                preferred_element_type=F32,
            )
            return carry

        lax.fori_loop(0, rows // step, one, 0)

    return call(
        body, shape_of((rows, tasks)), design, *blocks,
        scratch=[pltpu.VMEM((tasks, 4 * width), BF)],
    )


def joined(near, arrived, planes, corr=None):
    rows, tasks = near.shape
    outs = [shape_of((planes, rows // planes, tasks), BF)]
    if corr:
        outs += [shape_of((1, corr[0].shape[1])), shape_of((EXTRA, tasks))]

    def body(near, arrived, *refs):
        out = refs[len(corr)] if corr else refs[0]
        total = near[...] + arrived[...]
        out[...] = total.reshape(out.shape).astype(BF)
        if corr:
            c0, c1, c2, c3, _, steps, top = refs
            both = c0[...] + c1[...] + c2[...] + c3[...]
            column_squares = jnp.sum(both[tasks:], axis=0, keepdims=True)
            steps[...] = 0.5 / (1.0 + column_squares)
            top[...] = jnp.full(top.shape, jnp.max(lane_norms(both[:tasks])), F32)

    return call(body, outs, near, arrived, *(corr or []))


def turned_dot(right, left):
    return lax.dot_general(right, left, (((0,), (0,)), ((), ())), preferred_element_type=F32)


def grad_loop(near, right, design, total, block):
    planes = right.shape[0]
    group = 8
    step = group * block

    def one(i, carry):
        rows = right[pl.ds(i * group, group)].astype(F32)[:, :block]
        rows = rows.reshape(step, right.shape[2]).astype(BF)
        at = pl.multiple_of(half_start(near, planes * block) + i * step, step)
        total[...] += turned_dot(rows, design[pl.ds(at, step), :])
        return carry

    lax.fori_loop(0, planes // group, one, 0)


def grad_near(design, right, block):
    def body(design, right, total):
        total[...] = jnp.zeros_like(total)
        grad_loop(True, right, design, total, block)

    out = shape_of((right.shape[2], design.shape[1]))
    return call(body, out, design, right)


def top_of(right, block):
    pieces = right[:, block:, :].astype(F32)
    return jnp.max(jnp.sum(pieces, axis=1))


def grad_far(design, right, start, block, near=None):
    tasks, cols = start.shape
    width = cols // 4
    extra = 0 if near is None else EXTRA

    def body(design, right, start, *refs):
        outs, total = refs[-5:-1], refs[-1]
        total[...] = start[...]
        grad_loop(False, right, design, total, block)
        for k, out in enumerate(outs):
            at = block_at(k, width)
            out[:tasks, :] = total[:, pl.ds(at, width)]
        if extra:
            top = jnp.maximum(top_of(right, block), top_of(refs[0], block))
            for out in outs:
                out[tasks:, :] = jnp.full((extra, width), top, F32)

    outs = [shape_of((tasks + extra, width))] * 4
    args = [design, right, start] + ([] if near is None else [near])
    return call(body, outs, *args, scratch=[pltpu.VMEM((tasks, cols), F32)])


def residual_of(parts, own, at, stats=None, top=None):
    planes, block, tasks = parts.shape
    extra = 0 if top is None else EXTRA
    outs = [shape_of((planes, block + extra, tasks), BF), shape_of((1, 128))]

    def body(parts, own, given, copies, stats_out):
        fitted = jnp.sum(parts[...].astype(F32), axis=0)
        target = own[...].astype(F32)
        rounded = (target - fitted).astype(BF)
        wide = rounded.astype(F32)
        if extra:
            value = given[...]
            high = value.astype(BF).astype(F32)
            middle = (value - high).astype(BF).astype(F32)
            low = (value - high) - middle
            which = lax.broadcasted_iota(jnp.int32, value.shape, 0)
            tail = jnp.where(which == 0, high, jnp.where(which == 1, middle, low))
            tail = jnp.where(which < 3, tail, 0.0)
            rounded = jnp.concatenate([wide, tail], axis=0).astype(BF)
            row = jnp.zeros(stats_out.shape, F32)
        else:
            row = given[...]
        row = lane(row, at, jnp.sum(wide * wide))
        stats_out[...] = lane(row, at + 1, jnp.sum(wide * target))
        copies[...] = jnp.broadcast_to(rounded[None], copies.shape)

    return call(body, outs, parts, own, stats if top is None else top)


def penalty_of(top, index):
    return top / (8.0 + 4.0 * index[0].astype(F32))


def prox(parts, current, steps, mask, index, stats, at, out_dtype, tops=None):
    tasks, width = current.shape
    row_at = at // 8

    def body(own, r1, r2, r3, current, steps, mask, index, stats, *refs):
        new, sent, norms_out, stats_out, tops_out = refs[-5:]
        gradient = own[:tasks, :] + r1[:tasks, :] + r2[:tasks, :] + r3[:tasks, :]
        if tops is None:
            tops_out[...] = jnp.maximum(
                jnp.maximum(own[tasks:, :], r1[tasks:, :]),
                jnp.maximum(r2[tasks:, :], r3[tasks:, :]),
            )
        else:
            tops_out[...] = refs[0][...]
        norms = lane_norms(gradient)
        norms_out[...] = norms
        here = current[...]
        keep = mask[row_at : row_at + 1, pl.ds(block_at(0, width), width)].astype(F32)
        row = lane(stats[...], at + 2, jnp.sum(lane_norms(here)))
        row = lane(row, at + 3, jnp.max(norms))
        stats_out[...] = lane(row, at + 4, jnp.sum(1.0 - keep))
        penalty = penalty_of(tops_out[0:1, :], index)
        step = steps[...]
        moved = here + step * gradient
        moved_norms = lane_norms(moved)
        cutoff = step * penalty
        factor = jnp.maximum(moved_norms - cutoff, 0.0) / jnp.maximum(moved_norms, cutoff)
        value = (keep * factor) * moved
        new[...] = value
        sent[...] = value.astype(out_dtype)

    outs = [
        shape_of((tasks, width)),
        shape_of((tasks, width), out_dtype),
        shape_of((1, width)),
        shape_of(stats.shape),
        shape_of((EXTRA, width)),
    ]
    args = [*parts, current, steps, mask, index, stats] + ([] if tops is None else [tops])
    return call(body, outs, *args, smem=(7,))


def last_norms(parts, current, stats, n0, n1, at):
    width = n0.shape[1]

    def body(own, r1, r2, r3, current, stats, n0, n1, out):
        norms = lane_norms(own[...] + r1[...] + r2[...] + r3[...])
        row = lane(stats[...], at + 2, jnp.sum(lane_norms(current[...])))
        row = lane(row, at + 3, jnp.max(norms))
        wide = jnp.concatenate([row] * (width // row.shape[1]), axis=1)
        out[...] = jnp.concatenate([n0[...], n1[...], norms] + [wide] * 5, axis=0)

    return call(body, shape_of((8, width)), *parts, current, stats, n0, n1)


def of_samples(blocks, copies):
    def body(own, n1, n2, n3, out):
        rows = [ref[3:4, 0:128] for ref in (own, n1, n2, n3)]
        total = (rows[0] + rows[2]) + (rows[1] + rows[3])
        high = jnp.maximum(jnp.maximum(rows[0], rows[2]), jnp.maximum(rows[1], rows[3]))
        at = lax.broadcasted_iota(jnp.int32, total.shape, 1)
        out[...] = jnp.broadcast_to(jnp.where((at & 7) == 3, high, total), out.shape)

    return call(body, shape_of((copies, 128)), *blocks)


def finish(everyone, tops, index, blocks):
    width = blocks[0].shape[1]

    def body(everyone, tops, index, n0, n1, n2, n3, correlations, gaps, counts):
        values = everyone[...]
        sums = jnp.sum(values, axis=0, keepdims=True)
        highs = jnp.max(values, axis=0, keepdims=True)
        at_lane = lax.broadcasted_iota(jnp.int32, sums.shape, 1)

        def total(i):
            return jnp.full(sums.shape, jnp.sum(jnp.where(at_lane == i, sums, 0.0)), F32)

        penalty = penalty_of(tops[0:1, 0:128], index)
        row = jnp.zeros(sums.shape, F32)
        for t in range(ITERS + 1):
            at = 8 * t
            rr, ry, bn = total(at), total(at + 1), total(at + 2)
            top = jnp.max(jnp.where(at_lane == at + 3, highs, 0.0))
            scale = jnp.maximum(penalty, top)
            ratio = penalty / scale
            primal = 0.5 * rr + penalty * bn
            dual = ratio * ry - 0.5 * ratio * ratio * rr
            row = jnp.where(at_lane == t, (primal - dual) / (primal + 1.0), row)
            wide = jnp.concatenate([scale] * (width // 128), axis=1)
            for k, block in enumerate((n0, n1, n2, n3)):
                start = block_at(k, width)
                correlations[t : t + 1, pl.ds(start, width)] = block[t : t + 1, :] / wide
        for t in range(ITERS + 1):
            gaps[t] = jnp.sum(jnp.where(at_lane == t, row, 0.0))
        for t in range(ITERS):
            counts[t] = jnp.sum(jnp.where(at_lane == 8 * t + 4, sums, 0.0))

    outs = [shape_of((ITERS + 1, 4 * width)), shape_of((ITERS + 1,)), shape_of((ITERS,))]
    return call(body, outs, everyone, tops, index, *blocks, smem=(2,), smem_outs=(1, 2))


def turned_back(blocks):
    tasks, width = blocks[0].shape

    def body(c0, c1, c2, c3, out):
        for k, block in enumerate((c0, c1, c2, c3)):
            out[pl.ds(block_at(k, width), width), :] = block[...].T

    return call(body, shape_of((4 * width, tasks)), *blocks)


def to_owners(blocks):
    return [blocks[0]] + [shifted(blocks[k], "samp", k) for k in (1, 3, 2)]


def from_owners(value):
    got = {k: shifted(value, "samp", -k) for k in (1, 3, 2)}
    return [value, got[1], got[2], got[3]]


def plane_exchange(blocks):
    return lax.all_to_all(blocks, PLANE, split_axis=0, concat_axis=0, tiled=True)


def local(design, targets, warm_start, active_mask, penalty_index):
    rows, _ = design.shape
    half = rows // 2
    planes = lax.axis_size("y") * lax.axis_size("z")
    block = half // planes
    step = 8 * block
    blocks = tops = stats = None
    norms = []
    for t in range(ITERS + 1):
        if t == 0:
            *corr, design, own_targets = corr_first(design, targets, step, block)
            corr = to_owners(corr)
            (far,) = fit_warm(False, design, warm_start, half, step)
            arrived = shifted(far, "core", 1)
            near, current = fit_warm(True, design, warm_start, half, step)
            sums, steps, top = joined(near, arrived, planes, corr)
            copies, stats = residual_of(plane_exchange(sums), own_targets, 0, top=top)
        else:
            far = fit_rows(False, design, blocks, half, step)
            arrived = shifted(far, "core", 1)
            near = fit_rows(True, design, blocks, half, step)
            (sums,) = joined(near, arrived, planes)
            copies, stats = residual_of(plane_exchange(sums), own_targets, 8 * t, stats)
        near_rows = plane_exchange(copies)
        far_rows = shifted(near_rows, "core", 1)
        grad = grad_near(design, near_rows, block)
        shares = to_owners(
            grad_far(design, far_rows, grad, block, near_rows if t == 0 else None)
        )
        if t < ITERS:
            current, sent, own_norms, stats, tops = prox(
                shares, current, steps, active_mask, penalty_index, stats, 8 * t,
                BF if t + 1 < ITERS else F32, tops,
            )
            norms.append(own_norms)
            blocks = from_owners(sent)
            if t + 1 == ITERS:
                coefficients = turned_back(blocks)
        else:
            packed = last_norms(shares, current, stats, *norms, 8 * t)
    norm_blocks = from_owners(packed)
    features = planes * lax.axis_size("core")
    copies = of_samples(norm_blocks, features)
    everyone = lax.all_to_all(copies[:, None, :], FEAT, split_axis=0, concat_axis=0, tiled=True)
    correlations, gaps, counts = finish(
        everyone.reshape(copies.shape), tops, penalty_index, norm_blocks
    )
    return coefficients, correlations, gaps, counts


def solution(mesh):
    torus = Mesh(
        mesh.devices.reshape(4, 8, 2, mesh.shape["samp"]), ("y", "z", "core", "samp")
    )
    in_specs = (P("samp", FEAT), P("samp", None), P(FEAT, None), P(None, FEAT), P())
    out_specs = (P(FEAT, None), P(None, FEAT), P(), P())
    return jax.shard_map(
        local, mesh=torus, in_specs=in_specs, out_specs=out_specs, check_vma=False
    )
```

```python
import jax
import jax.numpy as jnp
from jax import lax
from jax.experimental import pallas as pl
from jax.experimental.pallas import tpu as pltpu
from jax.sharding import Mesh
from jax.sharding import PartitionSpec as P


ITERS = 2
FEAT = ("y", "z", "core")
ALL = ("y", "z", "core", "samp")
PLANE = ("y", "z")
BF = jnp.bfloat16
F32 = jnp.float32
EXTRA = 8
VMEM = pl.BlockSpec(memory_space=pltpu.VMEM)
SMEM = pl.BlockSpec(memory_space=pltpu.SMEM)


def shape_of(dims, dtype=F32):
    return jax.ShapeDtypeStruct(tuple(dims), dtype)


def call(body, outs, *args, smem=(), smem_outs=(), scratch=(), mib=4):
    single = not isinstance(outs, (list, tuple))
    shapes = [outs] if single else list(outs)
    out_specs = [SMEM if k in smem_outs else VMEM for k in range(len(shapes))]
    return pl.pallas_call(
        body,
        out_shape=shapes[0] if single else tuple(shapes),
        in_specs=[SMEM if k in smem else VMEM for k in range(len(args))],
        out_specs=out_specs[0] if single else tuple(out_specs),
        scratch_shapes=list(scratch),
        compiler_params=pltpu.CompilerParams(vmem_limit_bytes=mib << 20),
    )(*args)


def shifted(value, axis, by):
    n = lax.axis_size(axis)
    return lax.ppermute(value, axis, [(i, (i + by) % n) for i in range(n)])


def lane(row, index, value):
    at = lax.broadcasted_iota(jnp.int32, row.shape, 1)
    return jnp.where(at == index, value, row)


def lane_norms(value):
    return jnp.sqrt(jnp.sum(value * value, axis=0, keepdims=True))


def in_hbm(value):
    return pltpu.with_memory_space_constraint(value, pltpu.HBM)


def half_start(near, half):
    core = lax.axis_index("core")
    return (core if near else 1 - core) * half


def block_at(k, width):
    return pl.multiple_of(((lax.axis_index("samp") + k) & 3) * width, width)


def corr_first(design, targets, step, block):
    rows, cols = design.shape
    tasks = targets.shape[1]
    width = cols // 4
    count = rows // step

    def body(design, targets, o0, o1, o2, o3, held, own, right, total, squares, arrived):
        plane = lax.axis_index("y") * lax.axis_size("z") + lax.axis_index("z")
        at = pl.multiple_of(half_start(True, rows // 2) + plane * block, 8)
        mine = pltpu.make_async_copy(targets.at[pl.ds(at, block)], own, arrived.at[2 * count])

        def pieces(i):
            here = pl.ds(pl.multiple_of(i * step, step), step)
            return (
                pltpu.make_async_copy(targets.at[here], right.at[here], arrived.at[2 * i]),
                pltpu.make_async_copy(design.at[here], held.at[here], arrived.at[2 * i + 1]),
            )

        for i in range(count):
            for piece in pieces(i):
                piece.start()
        mine.start()
        total[...] = jnp.zeros_like(total)
        squares[...] = jnp.zeros_like(squares)

        def one(i, carry):
            for piece in pieces(i):
                piece.wait()
            here = pl.ds(pl.multiple_of(i * step, step), step)
            total[...] += turned_dot(right[here, :], held[here, :])

            def part(j, carry):
                inner = pl.multiple_of(i * step + j * 64, 64)
                wide = held[pl.ds(inner, 64), :].astype(F32)
                squares[...] += jnp.sum((wide * wide).reshape(8, 8, cols), axis=0)
                return carry

            lax.fori_loop(0, step // 64, part, 0)
            return carry

        lax.fori_loop(0, count, one, 0)
        mine.wait()
        for k, out in enumerate((o0, o1, o2, o3)):
            at = block_at(k, width)
            out[:tasks, :] = total[:, pl.ds(at, width)]
            out[tasks:, :] = squares[:, pl.ds(at, width)]

    hbm = pl.BlockSpec(memory_space=pltpu.HBM)
    return pl.pallas_call(
        body,
        out_shape=(
            *[shape_of((tasks + 8, width))] * 4,
            pltpu.VMEM(design.shape, design.dtype),
            shape_of((block, tasks), targets.dtype),
        ),
        in_specs=[hbm, hbm],
        out_specs=(VMEM,) * 6,
        scratch_shapes=[
            pltpu.VMEM((rows, tasks), targets.dtype),
            pltpu.VMEM((tasks, cols), F32),
            pltpu.VMEM((8, cols), F32),
            pltpu.SemaphoreType.DMA((2 * count + 1,)),
        ],
        compiler_params=pltpu.CompilerParams(vmem_limit_bytes=16 << 20),
        name="corr_first",
    )(in_hbm(design), in_hbm(targets))


def fit_warm(near, design, warm, rows, step):
    cols, tasks = warm.shape
    width = cols // 4

    def body(design, warm, out, *turned):
        right = warm[...].astype(BF)
        if near:
            turned[0][...] = warm[pl.ds(block_at(0, width), width), :].T

        def one(i, carry):
            at = pl.multiple_of(half_start(near, rows) + i * step, step)
            out[pl.ds(pl.multiple_of(i * step, step), step), :] = jnp.dot(
                design[pl.ds(at, step), :], right, preferred_element_type=F32
            )
            return carry

        lax.fori_loop(0, rows // step, one, 0)

    outs = [shape_of((rows, tasks))] + ([shape_of((tasks, width))] if near else [])
    return call(body, outs, design, warm)


def fit_rows(near, design, blocks, ks, rows, step, start=None):
    tasks, width = blocks[0].shape
    given = [] if start is None else [start]

    def body(design, *refs):
        *blocks, out, whole = refs
        for k, block in zip(range(len(ks)), blocks):
            whole[:, k * width : (k + 1) * width] = block[...].astype(BF)

        def one(i, carry):
            at = pl.multiple_of(half_start(near, rows) + i * step, step)
            here = pl.ds(pl.multiple_of(i * step, step), step)
            total = blocks[-1][here, :] if given else None
            for n, k in enumerate(ks):
                part = lax.dot_general(
                    design[pl.ds(at, step), pl.ds(block_at(k, width), width)],
                    whole[:, n * width : (n + 1) * width],
                    (((1,), (1,)), ((), ())),
                    preferred_element_type=F32,
                )
                total = part if total is None else total + part
            out[here, :] = total
            return carry

        lax.fori_loop(0, rows // step, one, 0)

    return call(
        body, shape_of((rows, tasks)), design, *[blocks[k] for k in ks], *given,
        scratch=[pltpu.VMEM((tasks, len(ks) * width), BF)],
    )


def fit_all(design, blocks, rows, step):
    tasks, width = blocks[0].shape

    def body(design, c0, c1, c2, c3, out, whole):
        for k, block in enumerate((c0, c1, c2, c3)):
            whole[:, pl.ds(block_at(k, width), width)] = block[...].astype(BF)

        def one(i, carry):
            at = pl.multiple_of(half_start(True, rows) + i * step, step)
            out[pl.ds(pl.multiple_of(i * step, step), step), :] = lax.dot_general(
                design[pl.ds(at, step), :],
                whole[...],
                (((1,), (1,)), ((), ())),
                preferred_element_type=F32,
            )
            return carry

        lax.fori_loop(0, rows // step, one, 0)

    return call(
        body, shape_of((rows, tasks)), design, *blocks,
        scratch=[pltpu.VMEM((tasks, 4 * width), BF)],
    )


def joined(near, arrived, planes, corr=None):
    rows, tasks = near.shape
    outs = [shape_of((planes, rows // planes, tasks), BF)]
    if corr:
        outs += [shape_of((1, corr[0].shape[1])), shape_of((EXTRA, tasks))]

    def body(near, arrived, *refs):
        out = refs[len(corr)] if corr else refs[0]
        total = near[...] + arrived[...]
        out[...] = total.reshape(out.shape).astype(BF)
        if corr:
            c0, c1, c2, c3, _, steps, top = refs
            both = c0[...] + c1[...] + c2[...] + c3[...]
            column_squares = jnp.sum(both[tasks:], axis=0, keepdims=True)
            steps[...] = 0.5 / (1.0 + column_squares)
            top[...] = jnp.full(top.shape, jnp.max(lane_norms(both[:tasks])), F32)

    return call(body, outs, near, arrived, *(corr or []))


def turned_dot(right, left):
    return lax.dot_general(right, left, (((0,), (0,)), ((), ())), preferred_element_type=F32)


def grad_loop(near, right, design, total, block):
    planes = right.shape[0]
    group = 8
    step = group * block

    def one(i, carry):
        rows = right[pl.ds(i * group, group)].astype(F32)[:, :block]
        rows = rows.reshape(step, right.shape[2]).astype(BF)
        at = pl.multiple_of(half_start(near, planes * block) + i * step, step)
        total[...] += turned_dot(rows, design[pl.ds(at, step), :])
        return carry

    lax.fori_loop(0, planes // group, one, 0)


def grad_near(design, right, block):
    def body(design, right, total):
        total[...] = jnp.zeros_like(total)
        grad_loop(True, right, design, total, block)

    out = shape_of((right.shape[2], design.shape[1]))
    return call(body, out, design, right)


def top_of(right, block):
    pieces = right[:, block:, :].astype(F32)
    return jnp.max(jnp.sum(pieces, axis=1))


def grad_far(ks, design, right, start, block, near=None):
    tasks, cols = start.shape
    width = cols // 4
    extra = 0 if near is None else EXTRA
    planes = right.shape[0]
    group = 8
    step = group * block

    def body(design, right, start, *refs):
        outs = refs[-len(ks) :]
        for k, out in zip(ks, outs):
            out[:tasks, :] = start[:, pl.ds(block_at(k, width), width)]

        def one(i, carry):
            rows = right[pl.ds(i * group, group)].astype(F32)[:, :block]
            rows = rows.reshape(step, tasks).astype(BF)
            at = pl.multiple_of(half_start(False, planes * block) + i * step, step)
            for k, out in zip(ks, outs):
                out[:tasks, :] += turned_dot(
                    rows, design[pl.ds(at, step), pl.ds(block_at(k, width), width)]
                )
            return carry

        lax.fori_loop(0, planes // group, one, 0)
        if extra:
            top = jnp.maximum(top_of(right, block), top_of(refs[0], block))
            for out in outs:
                out[tasks:, :] = jnp.full((extra, width), top, F32)

    outs = [shape_of((tasks + extra, width))] * len(ks)
    args = [design, right, start] + ([] if near is None else [near])
    return call(body, outs, *args)


def residual_of(parts, own, at, stats=None, top=None):
    planes, block, tasks = parts.shape
    extra = 0 if top is None else EXTRA
    outs = [shape_of((planes, block + extra, tasks), BF), shape_of((1, 128))]

    def body(parts, own, given, copies, stats_out):
        fitted = jnp.sum(parts[...].astype(F32), axis=0)
        target = own[...].astype(F32)
        rounded = (target - fitted).astype(BF)
        wide = rounded.astype(F32)
        if extra:
            value = given[...]
            high = value.astype(BF).astype(F32)
            middle = (value - high).astype(BF).astype(F32)
            low = (value - high) - middle
            which = lax.broadcasted_iota(jnp.int32, value.shape, 0)
            tail = jnp.where(which == 0, high, jnp.where(which == 1, middle, low))
            tail = jnp.where(which < 3, tail, 0.0)
            rounded = jnp.concatenate([wide, tail], axis=0).astype(BF)
            row = jnp.zeros(stats_out.shape, F32)
        else:
            row = given[...]
        row = lane(row, at, jnp.sum(wide * wide))
        stats_out[...] = lane(row, at + 1, jnp.sum(wide * target))
        copies[...] = jnp.broadcast_to(rounded[None], copies.shape)

    return call(body, outs, parts, own, stats if top is None else top)


def penalty_of(top, index):
    return top / (8.0 + 4.0 * index[0].astype(F32))


def prox(parts, current, steps, mask, index, stats, at, out_dtype, tops=None):
    tasks, width = current.shape
    row_at = at // 8

    def body(own, r1, r2, r3, current, steps, mask, index, stats, *refs):
        new, sent, norms_out, stats_out, tops_out = refs[-5:]
        gradient = own[:tasks, :] + r1[:tasks, :] + r2[:tasks, :] + r3[:tasks, :]
        if tops is None:
            tops_out[...] = jnp.maximum(
                jnp.maximum(own[tasks:, :], r1[tasks:, :]),
                jnp.maximum(r2[tasks:, :], r3[tasks:, :]),
            )
        else:
            tops_out[...] = refs[0][...]
        norms = lane_norms(gradient)
        norms_out[...] = norms
        here = current[...]
        keep = mask[row_at : row_at + 1, pl.ds(block_at(0, width), width)].astype(F32)
        row = lane(stats[...], at + 2, jnp.sum(lane_norms(here)))
        row = lane(row, at + 3, jnp.max(norms))
        stats_out[...] = lane(row, at + 4, jnp.sum(1.0 - keep))
        penalty = penalty_of(tops_out[0:1, :], index)
        step = steps[...]
        moved = here + step * gradient
        moved_norms = lane_norms(moved)
        cutoff = step * penalty
        factor = jnp.maximum(moved_norms - cutoff, 0.0) / jnp.maximum(moved_norms, cutoff)
        value = (keep * factor) * moved
        new[...] = value
        sent[...] = value.astype(out_dtype)

    outs = [
        shape_of((tasks, width)),
        shape_of((tasks, width), out_dtype),
        shape_of((1, width)),
        shape_of(stats.shape),
        shape_of((EXTRA, width)),
    ]
    args = [*parts, current, steps, mask, index, stats] + ([] if tops is None else [tops])
    return call(body, outs, *args, smem=(7,))


def last_norms(parts, current, stats, n0, n1, at, devices):
    def body(own, r1, r2, r3, current, stats, n0, n1, norms_out, copies):
        norms = lane_norms(own[...] + r1[...] + r2[...] + r3[...])
        norms_out[...] = jnp.concatenate([n0[...], n1[...], norms] + [norms] * 5, axis=0)
        row = lane(stats[...], at + 2, jnp.sum(lane_norms(current[...])))
        row = lane(row, at + 3, jnp.max(norms))
        copies[...] = jnp.broadcast_to(row, copies.shape)

    outs = [shape_of((8, n0.shape[1])), shape_of((devices, stats.shape[1]))]
    return call(body, outs, *parts, current, stats, n0, n1)


def finish(everyone, tops, index, blocks):
    width = blocks[0].shape[1]

    def body(everyone, tops, index, n0, n1, n2, n3, correlations, gaps, counts):
        values = everyone[...]
        sums = jnp.sum(values, axis=0, keepdims=True)
        highs = jnp.max(values, axis=0, keepdims=True)
        at_lane = lax.broadcasted_iota(jnp.int32, sums.shape, 1)

        def total(i):
            return jnp.full(sums.shape, jnp.sum(jnp.where(at_lane == i, sums, 0.0)), F32)

        penalty = penalty_of(tops[0:1, 0:128], index)
        row = jnp.zeros(sums.shape, F32)
        for t in range(ITERS + 1):
            at = 8 * t
            rr, ry, bn = total(at), total(at + 1), total(at + 2)
            top = jnp.max(jnp.where(at_lane == at + 3, highs, 0.0))
            scale = jnp.maximum(penalty, top)
            ratio = penalty / scale
            primal = 0.5 * rr + penalty * bn
            dual = ratio * ry - 0.5 * ratio * ratio * rr
            row = jnp.where(at_lane == t, (primal - dual) / (primal + 1.0), row)
            wide = jnp.concatenate([scale] * (width // 128), axis=1)
            for k, block in enumerate((n0, n1, n2, n3)):
                start = block_at(k, width)
                correlations[t : t + 1, pl.ds(start, width)] = block[t : t + 1, :] / wide
        for t in range(ITERS + 1):
            gaps[t] = jnp.sum(jnp.where(at_lane == t, row, 0.0))
        for t in range(ITERS):
            counts[t] = jnp.sum(jnp.where(at_lane == 8 * t + 4, sums, 0.0))

    outs = [shape_of((ITERS + 1, 4 * width)), shape_of((ITERS + 1,)), shape_of((ITERS,))]
    return call(body, outs, everyone, tops, index, *blocks, smem=(2,), smem_outs=(1, 2))


def turned_back(blocks):
    tasks, width = blocks[0].shape

    def body(c0, c1, c2, c3, out):
        for k, block in enumerate((c0, c1, c2, c3)):
            out[pl.ds(block_at(k, width), width), :] = block[...].T

    return call(body, shape_of((4 * width, tasks)), *blocks)


def to_owners(blocks):
    return [blocks[0]] + [shifted(blocks[k], "samp", k) for k in (1, 3, 2)]


def from_owners(value):
    got = {k: shifted(value, "samp", -k) for k in (1, 3, 2)}
    return [value, got[1], got[2], got[3]]


def plane_exchange(blocks):
    return lax.all_to_all(blocks, PLANE, split_axis=0, concat_axis=0, tiled=True)


def local(design, targets, warm_start, active_mask, penalty_index):
    rows, _ = design.shape
    half = rows // 2
    planes = lax.axis_size("y") * lax.axis_size("z")
    block = half // planes
    step = 8 * block
    devices = 1
    for axis in ALL:
        devices *= lax.axis_size(axis)

    state = {"far": None, "blocks": None, "stats": None, "tops": None, "norms": []}

    def iteration(t, design):
        if t == 0:
            *corr, design, own_targets = corr_first(design, targets, step, block)
            corr = to_owners(corr)
            (far,) = fit_warm(False, design, warm_start, half, step)
            arrived = shifted(far, "core", 1)
            near, state["current"] = fit_warm(True, design, warm_start, half, step)
            sums, state["steps"], top = joined(near, arrived, planes, corr)
            state["own_targets"] = own_targets
            copies, stats = residual_of(plane_exchange(sums), own_targets, 0, top=top)
        else:
            blocks = state["blocks"]
            arrived = shifted(state["far"], "core", 1)
            near = fit_all(design, blocks, half, step)
            (sums,) = joined(near, arrived, planes)
            copies, stats = residual_of(
                plane_exchange(sums), state["own_targets"], 8 * t, state["stats"]
            )
        near_rows = plane_exchange(copies)
        far_rows = shifted(near_rows, "core", 1)
        grad = grad_near(design, near_rows, block)
        given = near_rows if t == 0 else None
        b2, b1 = grad_far((2, 1), design, far_rows, grad, block, given)
        r2, r1 = shifted(b2, "samp", 2), shifted(b1, "samp", 1)
        b3, b0 = grad_far((3, 0), design, far_rows, grad, block, given)
        shares = [b0, r1, shifted(b3, "samp", 3), r2]
        if t == ITERS:
            return last_norms(shares, state["current"], stats, *state["norms"], 8 * t, devices)
        state["current"], sent, own_norms, state["stats"], state["tops"] = prox(
            shares, state["current"], state["steps"], active_mask, penalty_index, stats, 8 * t,
            BF if t + 1 < ITERS else F32, state["tops"],
        )
        state["norms"].append(own_norms)
        c1, c3 = shifted(sent, "samp", -1), shifted(sent, "samp", -3)
        c2 = shifted(sent, "samp", -2)
        blocks = state["blocks"] = [sent, c1, c2, c3]
        far = fit_rows(False, design, blocks, (0,), half, step)
        far = fit_rows(False, design, blocks, (1, 3), half, step, far)
        state["far"] = fit_rows(False, design, blocks, (2,), half, step, far)
        return design

    for t in range(ITERS):
        design = iteration(t, design)
    coefficients = turned_back(state["blocks"])
    packed, copies = iteration(ITERS, design)
    tops = state["tops"]
    norm_blocks = from_owners(packed)
    everyone = lax.all_to_all(copies[:, None, :], ALL, split_axis=0, concat_axis=0, tiled=True)
    correlations, gaps, counts = finish(
        everyone.reshape(copies.shape), tops, penalty_index, norm_blocks
    )
    return coefficients, correlations, gaps, counts


def solution(mesh):
    torus = Mesh(
        mesh.devices.reshape(4, 8, 2, mesh.shape["samp"]), ("y", "z", "core", "samp")
    )
    in_specs = (P("samp", FEAT), P("samp", None), P(FEAT, None), P(None, FEAT), P())
    out_specs = (P(FEAT, None), P(None, FEAT), P(), P())
    return jax.shard_map(
        local, mesh=torus, in_specs=in_specs, out_specs=out_specs, check_vma=False
    )
```

```python
import jax
import jax.numpy as jnp
from jax import lax
from jax.experimental import pallas as pl
from jax.experimental.pallas import tpu as pltpu
from jax.sharding import Mesh
from jax.sharding import PartitionSpec as P


ITERS = 2
FEAT = ("y", "z", "core")
ALL = ("y", "z", "core", "samp")
PLANE = ("y", "z")
BF = jnp.bfloat16
F32 = jnp.float32
EXTRA = 8
VMEM = pl.BlockSpec(memory_space=pltpu.VMEM)
SMEM = pl.BlockSpec(memory_space=pltpu.SMEM)


def shape_of(dims, dtype=F32):
    return jax.ShapeDtypeStruct(tuple(dims), dtype)


def call(body, outs, *args, smem=(), smem_outs=(), scratch=(), mib=4):
    single = not isinstance(outs, (list, tuple))
    shapes = [outs] if single else list(outs)
    out_specs = [SMEM if k in smem_outs else VMEM for k in range(len(shapes))]
    return pl.pallas_call(
        body,
        out_shape=shapes[0] if single else tuple(shapes),
        in_specs=[SMEM if k in smem else VMEM for k in range(len(args))],
        out_specs=out_specs[0] if single else tuple(out_specs),
        scratch_shapes=list(scratch),
        compiler_params=pltpu.CompilerParams(vmem_limit_bytes=mib << 20),
    )(*args)


def shifted(value, axis, by):
    n = lax.axis_size(axis)
    return lax.ppermute(value, axis, [(i, (i + by) % n) for i in range(n)])


def lane(row, index, value):
    at = lax.broadcasted_iota(jnp.int32, row.shape, 1)
    return jnp.where(at == index, value, row)


def lane_norms(value):
    return jnp.sqrt(jnp.sum(value * value, axis=0, keepdims=True))


def in_hbm(value):
    return pltpu.with_memory_space_constraint(value, pltpu.HBM)


def half_start(near, half):
    core = lax.axis_index("core")
    return (core if near else 1 - core) * half


def block_at(k, width):
    return pl.multiple_of(((lax.axis_index("samp") + k) & 3) * width, width)


def thirds(value, rows):
    value = jnp.broadcast_to(value, (rows, value.shape[1]))
    high = value.astype(BF).astype(F32)
    middle = (value - high).astype(BF).astype(F32)
    low = (value - high) - middle
    which = lax.broadcasted_iota(jnp.int32, value.shape, 0)
    spread = jnp.where(which == 0, high, jnp.where(which == 1, middle, low))
    return jnp.where(which < 3, spread, 0.0)


def corr_first(design, targets, step, block):
    rows, cols = design.shape
    tasks = targets.shape[1]
    width = cols // 4
    count = rows // step

    def body(design, targets, o0, o1, o2, o3, held, own, right, total, squares, arrived):
        plane = lax.axis_index("y") * lax.axis_size("z") + lax.axis_index("z")
        at = pl.multiple_of(half_start(True, rows // 2) + plane * block, 8)
        mine = pltpu.make_async_copy(targets.at[pl.ds(at, block)], own, arrived.at[2 * count])

        def pieces(i):
            here = pl.ds(pl.multiple_of(i * step, step), step)
            return (
                pltpu.make_async_copy(targets.at[here], right.at[here], arrived.at[2 * i]),
                pltpu.make_async_copy(design.at[here], held.at[here], arrived.at[2 * i + 1]),
            )

        for i in range(count):
            for piece in pieces(i):
                piece.start()
        mine.start()
        total[...] = jnp.zeros_like(total)
        squares[...] = jnp.zeros_like(squares)

        def one(i, carry):
            for piece in pieces(i):
                piece.wait()
            here = pl.ds(pl.multiple_of(i * step, step), step)
            total[...] += turned_dot(right[here, :], held[here, :])

            def part(j, carry):
                inner = pl.multiple_of(i * step + j * 64, 64)
                wide = held[pl.ds(inner, 64), :].astype(F32)
                squares[...] += jnp.sum((wide * wide).reshape(8, 8, cols), axis=0)
                return carry

            lax.fori_loop(0, step // 64, part, 0)
            return carry

        lax.fori_loop(0, count, one, 0)
        mine.wait()
        for k, out in enumerate((o0, o1, o2, o3)):
            at = block_at(k, width)
            out[:tasks, :] = total[:, pl.ds(at, width)].astype(out.dtype)
            row = jnp.sum(squares[:, pl.ds(at, width)], axis=0, keepdims=True)
            out[tasks:, :] = thirds(row, 2 * EXTRA).astype(out.dtype)

    hbm = pl.BlockSpec(memory_space=pltpu.HBM)
    return pl.pallas_call(
        body,
        out_shape=(
            shape_of((tasks + 2 * EXTRA, width)),
            *[shape_of((tasks + 2 * EXTRA, width), BF)] * 3,
            pltpu.VMEM(design.shape, design.dtype),
            shape_of((block, tasks), targets.dtype),
        ),
        in_specs=[hbm, hbm],
        out_specs=(VMEM,) * 6,
        scratch_shapes=[
            pltpu.VMEM((rows, tasks), targets.dtype),
            pltpu.VMEM((tasks, cols), F32),
            pltpu.VMEM((8, cols), F32),
            pltpu.SemaphoreType.DMA((2 * count + 1,)),
        ],
        compiler_params=pltpu.CompilerParams(vmem_limit_bytes=16 << 20),
        name="corr_first",
    )(in_hbm(design), in_hbm(targets))


def fit_warm(near, design, warm, rows, step):
    cols, tasks = warm.shape
    width = cols // 4

    def body(design, warm, out, *turned):
        right = warm[...].astype(BF)
        if near:
            turned[0][...] = warm[pl.ds(block_at(0, width), width), :].T

        def one(i, carry):
            at = pl.multiple_of(half_start(near, rows) + i * step, step)
            out[pl.ds(pl.multiple_of(i * step, step), step), :] = jnp.dot(
                design[pl.ds(at, step), :], right, preferred_element_type=F32
            )
            return carry

        lax.fori_loop(0, rows // step, one, 0)

    outs = [shape_of((rows, tasks))] + ([shape_of((tasks, width))] if near else [])
    return call(body, outs, design, warm)


def fit_rows(near, design, blocks, rows, step):
    tasks, width = blocks[0].shape

    def body(design, c0, c1, c2, c3, out, whole):
        for k, block in enumerate((c0, c1, c2, c3)):
            whole[:, pl.ds(block_at(k, width), width)] = block[...].astype(BF)

        def one(i, carry):
            at = pl.multiple_of(half_start(near, rows) + i * step, step)
            out[pl.ds(pl.multiple_of(i * step, step), step), :] = lax.dot_general(
                design[pl.ds(at, step), :],
                whole[...],
                (((1,), (1,)), ((), ())),
                preferred_element_type=F32,
            )
            return carry

        lax.fori_loop(0, rows // step, one, 0)

    return call(
        body, shape_of((rows, tasks)), design, *blocks,
        scratch=[pltpu.VMEM((tasks, 4 * width), BF)],
    )


def joined(near, arrived, planes, corr=None):
    rows, tasks = near.shape
    outs = [shape_of((planes, rows // planes, tasks), BF)]
    if corr:
        outs += [shape_of((1, corr[0].shape[1])), shape_of((EXTRA, tasks))]

    def body(near, arrived, *refs):
        out = refs[len(corr)] if corr else refs[0]
        total = near[...] + arrived[...]
        out[...] = total.reshape(out.shape).astype(BF)
        if corr:
            c0, c1, c2, c3, _, steps, top = refs
            both = c0[...]
            for share in (c1, c2, c3):
                both += share[...].astype(F32)
            column_squares = jnp.sum(both[tasks:], axis=0, keepdims=True)
            steps[...] = 0.5 / (1.0 + column_squares)
            top[...] = jnp.full(top.shape, jnp.max(lane_norms(both[:tasks])), F32)

    return call(body, outs, near, arrived, *(corr or []))


def turned_dot(right, left):
    return lax.dot_general(right, left, (((0,), (0,)), ((), ())), preferred_element_type=F32)


def grad_loop(near, right, design, total, block):
    planes = right.shape[0]
    group = 8
    step = group * block

    def one(i, carry):
        rows = right[pl.ds(i * group, group)].astype(F32)[:, :block]
        rows = rows.reshape(step, right.shape[2]).astype(BF)
        at = pl.multiple_of(half_start(near, planes * block) + i * step, step)
        total[...] += turned_dot(rows, design[pl.ds(at, step), :])
        return carry

    lax.fori_loop(0, planes // group, one, 0)


def grad_near(design, right, block):
    def body(design, right, total):
        total[...] = jnp.zeros_like(total)
        grad_loop(True, right, design, total, block)

    out = shape_of((right.shape[2], design.shape[1]))
    return call(body, out, design, right)


def top_of(right, block):
    pieces = right[:, block:, :].astype(F32)
    return jnp.max(jnp.sum(pieces, axis=1))


def grad_far(design, right, start, block, near=None, sent_as=F32):
    tasks, cols = start.shape
    width = cols // 4
    extra = 0 if near is None else EXTRA

    def body(design, right, start, *refs):
        outs, total = refs[-5:-1], refs[-1]
        total[...] = start[...]
        grad_loop(False, right, design, total, block)
        for k, out in enumerate(outs):
            at = block_at(k, width)
            out[:tasks, :] = total[:, pl.ds(at, width)].astype(out.dtype)
        if extra:
            top = jnp.maximum(top_of(right, block), top_of(refs[0], block))
            for out in outs:
                out[tasks:, :] = jnp.full((extra, width), top, F32)

    outs = [shape_of((tasks + extra, width))]
    outs += [shape_of((tasks + extra, width), sent_as)] * 3
    args = [design, right, start] + ([] if near is None else [near])
    return call(body, outs, *args, scratch=[pltpu.VMEM((tasks, cols), F32)])


def residual_of(parts, own, at, stats=None, top=None):
    planes, block, tasks = parts.shape
    extra = 0 if top is None else EXTRA
    outs = [shape_of((planes, block + extra, tasks), BF), shape_of((1, 128))]

    def body(parts, own, given, copies, stats_out):
        fitted = jnp.sum(parts[...].astype(F32), axis=0)
        target = own[...].astype(F32)
        rounded = (target - fitted).astype(BF)
        wide = rounded.astype(F32)
        if extra:
            value = given[...]
            high = value.astype(BF).astype(F32)
            middle = (value - high).astype(BF).astype(F32)
            low = (value - high) - middle
            which = lax.broadcasted_iota(jnp.int32, value.shape, 0)
            tail = jnp.where(which == 0, high, jnp.where(which == 1, middle, low))
            tail = jnp.where(which < 3, tail, 0.0)
            rounded = jnp.concatenate([wide, tail], axis=0).astype(BF)
            row = jnp.zeros(stats_out.shape, F32)
        else:
            row = given[...]
        row = lane(row, at, jnp.sum(wide * wide))
        stats_out[...] = lane(row, at + 1, jnp.sum(wide * target))
        copies[...] = jnp.broadcast_to(rounded[None], copies.shape)

    return call(body, outs, parts, own, stats if top is None else top)


def penalty_of(top, index):
    return top / (8.0 + 4.0 * index[0].astype(F32))


def prox(parts, current, steps, mask, index, stats, at, out_dtype, tops=None):
    tasks, width = current.shape
    row_at = at // 8

    def body(own, r1, r2, r3, current, steps, mask, index, stats, *refs):
        new, sent, norms_out, stats_out, tops_out = refs[-5:]
        gradient = own[:tasks, :] + r1[:tasks, :] + r2[:tasks, :] + r3[:tasks, :]
        if tops is None:
            tops_out[...] = jnp.maximum(
                jnp.maximum(own[tasks:, :], r1[tasks:, :]),
                jnp.maximum(r2[tasks:, :], r3[tasks:, :]),
            )
        else:
            tops_out[...] = refs[0][...]
        norms = lane_norms(gradient)
        norms_out[...] = norms
        here = current[...]
        keep = mask[row_at : row_at + 1, pl.ds(block_at(0, width), width)].astype(F32)
        row = lane(stats[...], at + 2, jnp.sum(lane_norms(here)))
        row = lane(row, at + 3, jnp.max(norms))
        stats_out[...] = lane(row, at + 4, jnp.sum(1.0 - keep))
        penalty = penalty_of(tops_out[0:1, :], index)
        step = steps[...]
        moved = here + step * gradient
        moved_norms = lane_norms(moved)
        cutoff = step * penalty
        factor = jnp.maximum(moved_norms - cutoff, 0.0) / jnp.maximum(moved_norms, cutoff)
        value = (keep * factor) * moved
        new[...] = value
        sent[...] = value.astype(out_dtype)

    outs = [
        shape_of((tasks, width)),
        shape_of((tasks, width), out_dtype),
        shape_of((1, width)),
        shape_of(stats.shape),
        shape_of((EXTRA, width)),
    ]
    args = [*parts, current, steps, mask, index, stats] + ([] if tops is None else [tops])
    return call(body, outs, *args, smem=(7,))


def last_norms(parts, current, stats, n0, n1, at, devices):
    def body(own, r1, r2, r3, current, stats, n0, n1, norms_out, copies):
        gradient = own[...]
        for share in (r1, r2, r3):
            gradient += share[...].astype(F32)
        norms = lane_norms(gradient)
        norms_out[...] = jnp.concatenate([n0[...], n1[...], norms] + [norms] * 5, axis=0)
        row = lane(stats[...], at + 2, jnp.sum(lane_norms(current[...])))
        row = lane(row, at + 3, jnp.max(norms))
        copies[...] = jnp.broadcast_to(row, copies.shape)

    outs = [shape_of((8, n0.shape[1])), shape_of((devices, stats.shape[1]))]
    return call(body, outs, *parts, current, stats, n0, n1)


def finish(everyone, tops, index, blocks):
    width = blocks[0].shape[1]

    def body(everyone, tops, index, n0, n1, n2, n3, correlations, gaps, counts):
        values = everyone[...]
        sums = jnp.sum(values, axis=0, keepdims=True)
        highs = jnp.max(values, axis=0, keepdims=True)
        at_lane = lax.broadcasted_iota(jnp.int32, sums.shape, 1)

        def total(i):
            return jnp.full(sums.shape, jnp.sum(jnp.where(at_lane == i, sums, 0.0)), F32)

        penalty = penalty_of(tops[0:1, 0:128], index)
        row = jnp.zeros(sums.shape, F32)
        for t in range(ITERS + 1):
            at = 8 * t
            rr, ry, bn = total(at), total(at + 1), total(at + 2)
            top = jnp.max(jnp.where(at_lane == at + 3, highs, 0.0))
            scale = jnp.maximum(penalty, top)
            ratio = penalty / scale
            primal = 0.5 * rr + penalty * bn
            dual = ratio * ry - 0.5 * ratio * ratio * rr
            row = jnp.where(at_lane == t, (primal - dual) / (primal + 1.0), row)
            wide = jnp.concatenate([scale] * (width // 128), axis=1)
            for k, block in enumerate((n0, n1, n2, n3)):
                start = block_at(k, width)
                correlations[t : t + 1, pl.ds(start, width)] = block[t : t + 1, :] / wide
        for t in range(ITERS + 1):
            gaps[t] = jnp.sum(jnp.where(at_lane == t, row, 0.0))
        for t in range(ITERS):
            counts[t] = jnp.sum(jnp.where(at_lane == 8 * t + 4, sums, 0.0))

    outs = [shape_of((ITERS + 1, 4 * width)), shape_of((ITERS + 1,)), shape_of((ITERS,))]
    return call(body, outs, everyone, tops, index, *blocks, smem=(2,), smem_outs=(1, 2))


def turned_back(blocks):
    tasks, width = blocks[0].shape

    def body(c0, c1, c2, c3, out):
        for k, block in enumerate((c0, c1, c2, c3)):
            out[pl.ds(block_at(k, width), width), :] = block[...].T

    return call(body, shape_of((4 * width, tasks)), *blocks)


def to_owners(blocks):
    return [blocks[0]] + [shifted(blocks[k], "samp", k) for k in (1, 3, 2)]


def from_owners(value):
    got = {k: shifted(value, "samp", -k) for k in (1, 3, 2)}
    return [value, got[1], got[2], got[3]]


def plane_exchange(blocks):
    return lax.all_to_all(blocks, PLANE, split_axis=0, concat_axis=0, tiled=True)


def local(design, targets, warm_start, active_mask, penalty_index):
    rows, _ = design.shape
    half = rows // 2
    planes = lax.axis_size("y") * lax.axis_size("z")
    block = half // planes
    step = 8 * block
    devices = 1
    for axis in ALL:
        devices *= lax.axis_size(axis)

    blocks = tops = stats = None
    norms = []
    for t in range(ITERS + 1):
        if t == 0:
            *corr, design, own_targets = corr_first(design, targets, step, block)
            corr = to_owners(corr)
            (far,) = fit_warm(False, design, warm_start, half, step)
            arrived = shifted(far, "core", 1)
            near, current = fit_warm(True, design, warm_start, half, step)
            sums, steps, top = joined(near, arrived, planes, corr)
            copies, stats = residual_of(plane_exchange(sums), own_targets, 0, top=top)
        else:
            far = fit_rows(False, design, blocks, half, step)
            arrived = shifted(far, "core", 1)
            near = fit_rows(True, design, blocks, half, step)
            (sums,) = joined(near, arrived, planes)
            copies, stats = residual_of(plane_exchange(sums), own_targets, 8 * t, stats)
        near_rows = plane_exchange(copies)
        far_rows = shifted(near_rows, "core", 1)
        grad = grad_near(design, near_rows, block)
        shares = to_owners(
            grad_far(
                design, far_rows, grad, block, near_rows if t == 0 else None,
                F32 if t < ITERS else BF,
            )
        )
        if t < ITERS:
            current, sent, own_norms, stats, tops = prox(
                shares, current, steps, active_mask, penalty_index, stats, 8 * t,
                BF if t + 1 < ITERS else F32, tops,
            )
            norms.append(own_norms)
            blocks = from_owners(sent)
            if t + 1 == ITERS:
                coefficients = turned_back(blocks)
        else:
            packed, copies = last_norms(shares, current, stats, *norms, 8 * t, devices)
    norm_blocks = from_owners(packed)
    everyone = lax.all_to_all(copies[:, None, :], ALL, split_axis=0, concat_axis=0, tiled=True)
    correlations, gaps, counts = finish(
        everyone.reshape(copies.shape), tops, penalty_index, norm_blocks
    )
    return coefficients, correlations, gaps, counts


def solution(mesh):
    torus = Mesh(
        mesh.devices.reshape(4, 8, 2, mesh.shape["samp"]), ("y", "z", "core", "samp")
    )
    in_specs = (P("samp", FEAT), P("samp", None), P(FEAT, None), P(None, FEAT), P())
    out_specs = (P(FEAT, None), P(None, FEAT), P(), P())
    return jax.shard_map(
        local, mesh=torus, in_specs=in_specs, out_specs=out_specs, check_vma=False
    )
```

```python
import jax
import jax.numpy as jnp
from jax import lax
from jax.experimental import pallas as pl
from jax.experimental.pallas import tpu as pltpu
from jax.sharding import Mesh
from jax.sharding import PartitionSpec as P


ITERS = 2
FEAT = ("y", "z", "core")
ALL = ("y", "z", "core", "samp")
PLANE = ("y", "z")
BF = jnp.bfloat16
F32 = jnp.float32
EXTRA = 8
VMEM = pl.BlockSpec(memory_space=pltpu.VMEM)
SMEM = pl.BlockSpec(memory_space=pltpu.SMEM)


def shape_of(dims, dtype=F32):
    return jax.ShapeDtypeStruct(tuple(dims), dtype)


def call(body, outs, *args, smem=(), smem_outs=(), scratch=(), mib=4):
    single = not isinstance(outs, (list, tuple))
    shapes = [outs] if single else list(outs)
    out_specs = [SMEM if k in smem_outs else VMEM for k in range(len(shapes))]
    return pl.pallas_call(
        body,
        out_shape=shapes[0] if single else tuple(shapes),
        in_specs=[SMEM if k in smem else VMEM for k in range(len(args))],
        out_specs=out_specs[0] if single else tuple(out_specs),
        scratch_shapes=list(scratch),
        compiler_params=pltpu.CompilerParams(vmem_limit_bytes=mib << 20),
    )(*args)


def shifted(value, axis, by):
    n = lax.axis_size(axis)
    return lax.ppermute(value, axis, [(i, (i + by) % n) for i in range(n)])


def lane(row, index, value):
    at = lax.broadcasted_iota(jnp.int32, row.shape, 1)
    return jnp.where(at == index, value, row)


def lane_norms(value):
    return jnp.sqrt(jnp.sum(value * value, axis=0, keepdims=True))


def in_hbm(value):
    return pltpu.with_memory_space_constraint(value, pltpu.HBM)


def half_start(near, half):
    core = lax.axis_index("core")
    return (core if near else 1 - core) * half


def block_at(k, width):
    return pl.multiple_of(((lax.axis_index("samp") + k) & 3) * width, width)


def thirds(value, rows):
    value = jnp.broadcast_to(value, (rows, value.shape[1]))
    high = value.astype(BF).astype(F32)
    middle = (value - high).astype(BF).astype(F32)
    low = (value - high) - middle
    which = lax.broadcasted_iota(jnp.int32, value.shape, 0)
    spread = jnp.where(which == 0, high, jnp.where(which == 1, middle, low))
    return jnp.where(which < 3, spread, 0.0)


def corr_first(design, targets, step, block):
    rows, cols = design.shape
    tasks = targets.shape[1]
    width = cols // 4
    count = rows // step

    def body(design, targets, o0, o1, o2, o3, held, own, right, total, squares, arrived):
        plane = lax.axis_index("y") * lax.axis_size("z") + lax.axis_index("z")
        at = pl.multiple_of(half_start(True, rows // 2) + plane * block, 8)
        mine = pltpu.make_async_copy(targets.at[pl.ds(at, block)], own, arrived.at[2 * count])

        def pieces(i):
            here = pl.ds(pl.multiple_of(i * step, step), step)
            return (
                pltpu.make_async_copy(targets.at[here], right.at[here], arrived.at[2 * i]),
                pltpu.make_async_copy(design.at[here], held.at[here], arrived.at[2 * i + 1]),
            )

        for i in range(count):
            for piece in pieces(i):
                piece.start()
        mine.start()
        total[...] = jnp.zeros_like(total)
        squares[...] = jnp.zeros_like(squares)

        def one(i, carry):
            for piece in pieces(i):
                piece.wait()
            here = pl.ds(pl.multiple_of(i * step, step), step)
            total[...] += turned_dot(right[here, :], held[here, :])

            def part(j, carry):
                inner = pl.multiple_of(i * step + j * 64, 64)
                wide = held[pl.ds(inner, 64), :].astype(F32)
                squares[...] += jnp.sum((wide * wide).reshape(8, 8, cols), axis=0)
                return carry

            lax.fori_loop(0, step // 64, part, 0)
            return carry

        lax.fori_loop(0, count, one, 0)
        mine.wait()
        for k, out in enumerate((o0, o1, o2, o3)):
            at = block_at(k, width)
            out[:tasks, :] = total[:, pl.ds(at, width)].astype(out.dtype)
            row = jnp.sum(squares[:, pl.ds(at, width)], axis=0, keepdims=True)
            out[tasks:, :] = thirds(row, 2 * EXTRA).astype(out.dtype)

    hbm = pl.BlockSpec(memory_space=pltpu.HBM)
    return pl.pallas_call(
        body,
        out_shape=(
            shape_of((tasks + 2 * EXTRA, width)),
            *[shape_of((tasks + 2 * EXTRA, width), BF)] * 3,
            pltpu.VMEM(design.shape, design.dtype),
            shape_of((block, tasks), targets.dtype),
        ),
        in_specs=[hbm, hbm],
        out_specs=(VMEM,) * 6,
        scratch_shapes=[
            pltpu.VMEM((rows, tasks), targets.dtype),
            pltpu.VMEM((tasks, cols), F32),
            pltpu.VMEM((8, cols), F32),
            pltpu.SemaphoreType.DMA((2 * count + 1,)),
        ],
        compiler_params=pltpu.CompilerParams(vmem_limit_bytes=16 << 20),
        name="corr_first",
    )(in_hbm(design), in_hbm(targets))


def fit_warm(near, design, warm, rows, step):
    cols, tasks = warm.shape
    width = cols // 4

    def body(design, warm, out, *turned):
        right = warm[...].astype(BF)
        if near:
            turned[0][...] = warm[pl.ds(block_at(0, width), width), :].T

        def one(i, carry):
            at = pl.multiple_of(half_start(near, rows) + i * step, step)
            out[pl.ds(pl.multiple_of(i * step, step), step), :] = jnp.dot(
                design[pl.ds(at, step), :], right, preferred_element_type=F32
            )
            return carry

        lax.fori_loop(0, rows // step, one, 0)

    outs = [shape_of((rows, tasks))] + ([shape_of((tasks, width))] if near else [])
    return call(body, outs, design, warm)


def fit_rows(near, design, blocks, rows, step):
    tasks, width = blocks[0].shape

    def body(design, c0, c1, c2, c3, out, whole):
        for k, block in enumerate((c0, c1, c2, c3)):
            whole[:, pl.ds(block_at(k, width), width)] = block[...].astype(BF)

        def one(i, carry):
            at = pl.multiple_of(half_start(near, rows) + i * step, step)
            out[pl.ds(pl.multiple_of(i * step, step), step), :] = lax.dot_general(
                design[pl.ds(at, step), :],
                whole[...],
                (((1,), (1,)), ((), ())),
                preferred_element_type=F32,
            )
            return carry

        lax.fori_loop(0, rows // step, one, 0)

    return call(
        body, shape_of((rows, tasks)), design, *blocks,
        scratch=[pltpu.VMEM((tasks, 4 * width), BF)],
    )


def joined(near, arrived, planes, corr=None):
    rows, tasks = near.shape
    outs = [shape_of((planes, rows // planes, tasks), BF)]
    if corr:
        outs += [shape_of((1, corr[0].shape[1])), shape_of((EXTRA, tasks))]

    def body(near, arrived, *refs):
        out = refs[len(corr)] if corr else refs[0]
        total = near[...] + arrived[...]
        out[...] = total.reshape(out.shape).astype(BF)
        if corr:
            c0, c1, c2, c3, _, steps, top = refs
            both = c0[...]
            for share in (c1, c2, c3):
                both += share[...].astype(F32)
            column_squares = jnp.sum(both[tasks:], axis=0, keepdims=True)
            steps[...] = 0.5 / (1.0 + column_squares)
            top[...] = jnp.full(top.shape, jnp.max(lane_norms(both[:tasks])), F32)

    return call(body, outs, near, arrived, *(corr or []))


def turned_dot(right, left):
    return lax.dot_general(right, left, (((0,), (0,)), ((), ())), preferred_element_type=F32)


def grad_loop(near, right, design, total, block):
    planes = right.shape[0]
    group = 8
    step = group * block

    def one(i, carry):
        rows = right[pl.ds(i * group, group)].astype(F32)[:, :block]
        rows = rows.reshape(step, right.shape[2]).astype(BF)
        at = pl.multiple_of(half_start(near, planes * block) + i * step, step)
        total[...] += turned_dot(rows, design[pl.ds(at, step), :])
        return carry

    lax.fori_loop(0, planes // group, one, 0)


def grad_near(design, right, block):
    def body(design, right, total):
        total[...] = jnp.zeros_like(total)
        grad_loop(True, right, design, total, block)

    out = shape_of((right.shape[2], design.shape[1]))
    return call(body, out, design, right)


def top_of(right, block):
    pieces = right[:, block:, :].astype(F32)
    return jnp.max(jnp.sum(pieces, axis=1))


def grad_far(design, right, start, block, near=None, sent_as=F32):
    tasks, cols = start.shape
    width = cols // 4
    extra = 0 if near is None else EXTRA

    def body(design, right, start, *refs):
        outs, total = refs[-5:-1], refs[-1]
        total[...] = start[...]
        grad_loop(False, right, design, total, block)
        for k, out in enumerate(outs):
            at = block_at(k, width)
            out[:tasks, :] = total[:, pl.ds(at, width)].astype(out.dtype)
        if extra:
            top = jnp.maximum(top_of(right, block), top_of(refs[0], block))
            for out in outs:
                out[tasks:, :] = jnp.full((extra, width), top, F32)

    outs = [shape_of((tasks + extra, width))]
    outs += [shape_of((tasks + extra, width), sent_as)] * 3
    args = [design, right, start] + ([] if near is None else [near])
    return call(body, outs, *args, scratch=[pltpu.VMEM((tasks, cols), F32)])


def residual_of(parts, own, at, stats=None, top=None):
    planes, block, tasks = parts.shape
    extra = 0 if top is None else EXTRA
    outs = [shape_of((planes, block + extra, tasks), BF), shape_of((1, 128))]

    def body(parts, own, given, copies, stats_out):
        fitted = jnp.sum(parts[...].astype(F32), axis=0)
        target = own[...].astype(F32)
        rounded = (target - fitted).astype(BF)
        wide = rounded.astype(F32)
        if extra:
            value = given[...]
            high = value.astype(BF).astype(F32)
            middle = (value - high).astype(BF).astype(F32)
            low = (value - high) - middle
            which = lax.broadcasted_iota(jnp.int32, value.shape, 0)
            tail = jnp.where(which == 0, high, jnp.where(which == 1, middle, low))
            tail = jnp.where(which < 3, tail, 0.0)
            rounded = jnp.concatenate([wide, tail], axis=0).astype(BF)
            row = jnp.zeros(stats_out.shape, F32)
        else:
            row = given[...]
        row = lane(row, at, jnp.sum(wide * wide))
        stats_out[...] = lane(row, at + 1, jnp.sum(wide * target))
        copies[...] = jnp.broadcast_to(rounded[None], copies.shape)

    return call(body, outs, parts, own, stats if top is None else top)


def penalty_of(top, index):
    return top / (8.0 + 4.0 * index[0].astype(F32))


def prox(parts, current, steps, mask, index, stats, at, out_dtype, tops=None):
    tasks, width = current.shape
    row_at = at // 8

    def body(own, r1, r2, r3, current, steps, mask, index, stats, *refs):
        new, sent, norms_out, stats_out, tops_out = refs[-5:]
        gradient = own[:tasks, :] + r1[:tasks, :] + r2[:tasks, :] + r3[:tasks, :]
        if tops is None:
            tops_out[...] = jnp.maximum(
                jnp.maximum(own[tasks:, :], r1[tasks:, :]),
                jnp.maximum(r2[tasks:, :], r3[tasks:, :]),
            )
        else:
            tops_out[...] = refs[0][...]
        norms = lane_norms(gradient)
        norms_out[...] = norms
        here = current[...]
        keep = mask[row_at : row_at + 1, pl.ds(block_at(0, width), width)].astype(F32)
        row = lane(stats[...], at + 2, jnp.sum(lane_norms(here)))
        row = lane(row, at + 3, jnp.max(norms))
        stats_out[...] = lane(row, at + 4, jnp.sum(1.0 - keep))
        penalty = penalty_of(tops_out[0:1, :], index)
        step = steps[...]
        moved = here + step * gradient
        moved_norms = lane_norms(moved)
        cutoff = step * penalty
        factor = jnp.maximum(moved_norms - cutoff, 0.0) / jnp.maximum(moved_norms, cutoff)
        value = (keep * factor) * moved
        new[...] = value
        sent[...] = value.astype(out_dtype)

    outs = [
        shape_of((tasks, width)),
        shape_of((tasks, width), out_dtype),
        shape_of((1, width)),
        shape_of(stats.shape),
        shape_of((EXTRA, width)),
    ]
    args = [*parts, current, steps, mask, index, stats] + ([] if tops is None else [tops])
    return call(body, outs, *args, smem=(7,))


def last_norms(parts, current, stats, n0, n1, at, devices):
    tasks, width = current.shape

    def body(own, r1, r2, r3, current, stats, n0, n1, packed, copies):
        gradient = own[...]
        for share in (r1, r2, r3):
            gradient += share[...].astype(F32)
        norms = lane_norms(gradient)
        out_rows = jnp.concatenate([n0[...], n1[...], norms] + [norms] * 5, axis=0)
        packed[:tasks, :] = current[...]
        packed[tasks:, :] = out_rows
        row = lane(stats[...], at + 2, jnp.sum(lane_norms(current[...])))
        row = lane(row, at + 3, jnp.max(norms))
        copies[...] = jnp.broadcast_to(row, copies.shape)

    outs = [shape_of((tasks + 8, width)), shape_of((devices, stats.shape[1]))]
    return call(body, outs, *parts, current, stats, n0, n1)


def finish(everyone, tops, index, blocks):
    width = blocks[0].shape[1]

    def body(everyone, tops, index, n0, n1, n2, n3, correlations, gaps, counts):
        values = everyone[...]
        sums = jnp.sum(values, axis=0, keepdims=True)
        highs = jnp.max(values, axis=0, keepdims=True)
        at_lane = lax.broadcasted_iota(jnp.int32, sums.shape, 1)

        def total(i):
            return jnp.full(sums.shape, jnp.sum(jnp.where(at_lane == i, sums, 0.0)), F32)

        penalty = penalty_of(tops[0:1, 0:128], index)
        row = jnp.zeros(sums.shape, F32)
        for t in range(ITERS + 1):
            at = 8 * t
            rr, ry, bn = total(at), total(at + 1), total(at + 2)
            top = jnp.max(jnp.where(at_lane == at + 3, highs, 0.0))
            scale = jnp.maximum(penalty, top)
            ratio = penalty / scale
            primal = 0.5 * rr + penalty * bn
            dual = ratio * ry - 0.5 * ratio * ratio * rr
            row = jnp.where(at_lane == t, (primal - dual) / (primal + 1.0), row)
            wide = jnp.concatenate([scale] * (width // 128), axis=1)
            for k, block in enumerate((n0, n1, n2, n3)):
                start = block_at(k, width)
                row_at = block.shape[0] - 8 + t
                correlations[t : t + 1, pl.ds(start, width)] = block[row_at : row_at + 1, :] / wide
        for t in range(ITERS + 1):
            gaps[t] = jnp.sum(jnp.where(at_lane == t, row, 0.0))
        for t in range(ITERS):
            counts[t] = jnp.sum(jnp.where(at_lane == 8 * t + 4, sums, 0.0))

    outs = [shape_of((ITERS + 1, 4 * width)), shape_of((ITERS + 1,)), shape_of((ITERS,))]
    return call(body, outs, everyone, tops, index, *blocks, smem=(2,), smem_outs=(1, 2))


def turned_back(blocks):
    tasks, width = blocks[0].shape[0] - 8, blocks[0].shape[1]

    def body(c0, c1, c2, c3, out):
        for k, block in enumerate((c0, c1, c2, c3)):
            out[pl.ds(block_at(k, width), width), :] = block[:tasks, :].T

    return call(body, shape_of((4 * width, tasks)), *blocks)


def to_owners(blocks):
    return [blocks[0]] + [shifted(blocks[k], "samp", k) for k in (1, 3, 2)]


def from_owners(value):
    got = {k: shifted(value, "samp", -k) for k in (1, 3, 2)}
    return [value, got[1], got[2], got[3]]


def plane_exchange(blocks):
    return lax.all_to_all(blocks, PLANE, split_axis=0, concat_axis=0, tiled=True)


def local(design, targets, warm_start, active_mask, penalty_index):
    rows, _ = design.shape
    half = rows // 2
    planes = lax.axis_size("y") * lax.axis_size("z")
    block = half // planes
    step = 8 * block
    devices = 1
    for axis in ALL:
        devices *= lax.axis_size(axis)

    blocks = tops = stats = None
    norms = []
    for t in range(ITERS + 1):
        if t == 0:
            *corr, design, own_targets = corr_first(design, targets, step, block)
            corr = to_owners(corr)
            (far,) = fit_warm(False, design, warm_start, half, step)
            arrived = shifted(far, "core", 1)
            near, current = fit_warm(True, design, warm_start, half, step)
            sums, steps, top = joined(near, arrived, planes, corr)
            copies, stats = residual_of(plane_exchange(sums), own_targets, 0, top=top)
        else:
            far = fit_rows(False, design, blocks, half, step)
            arrived = shifted(far, "core", 1)
            near = fit_rows(True, design, blocks, half, step)
            (sums,) = joined(near, arrived, planes)
            copies, stats = residual_of(plane_exchange(sums), own_targets, 8 * t, stats)
        near_rows = plane_exchange(copies)
        far_rows = shifted(near_rows, "core", 1)
        grad = grad_near(design, near_rows, block)
        shares = to_owners(
            grad_far(
                design, far_rows, grad, block, near_rows if t == 0 else None,
                F32 if t < ITERS else BF,
            )
        )
        if t < ITERS:
            current, sent, own_norms, stats, tops = prox(
                shares, current, steps, active_mask, penalty_index, stats, 8 * t,
                BF, tops,
            )
            norms.append(own_norms)
            blocks = from_owners(sent)
        else:
            packed, copies = last_norms(shares, current, stats, *norms, 8 * t, devices)
    norm_blocks = from_owners(packed)
    coefficients = turned_back(norm_blocks)
    everyone = lax.all_to_all(copies[:, None, :], ALL, split_axis=0, concat_axis=0, tiled=True)
    correlations, gaps, counts = finish(
        everyone.reshape(copies.shape), tops, penalty_index, norm_blocks
    )
    return coefficients, correlations, gaps, counts


def solution(mesh):
    torus = Mesh(
        mesh.devices.reshape(4, 8, 2, mesh.shape["samp"]), ("y", "z", "core", "samp")
    )
    in_specs = (P("samp", FEAT), P("samp", None), P(FEAT, None), P(None, FEAT), P())
    out_specs = (P(FEAT, None), P(None, FEAT), P(), P())
    return jax.shard_map(
        local, mesh=torus, in_specs=in_specs, out_specs=out_specs, check_vma=False
    )
```
